32 devices in a mesh: grp: 8 (over z, y), blk: 4 (over x, core).
Axes of the slice: x: 2, y: 2, z: 4, core: 2. Of those that a mesh axis runs over, the one named last changes fastest.
Arguments:
- query: bfloat16 [4096, 512], P(('grp', 'blk')), may hold values from -6 to 6
- key: bfloat16 [4096, 512], P(('grp', 'blk')), may hold values from -6 to 6
- value: bfloat16 [4096, 512], P(('grp', 'blk')), may hold values from -6 to 6
- gate_u: bfloat16 [4096, 512], P(('grp', 'blk')), may hold values from -6 to 6
- out_grad: bfloat16 [4096, 1024], P(('grp', 'blk')), may hold values from -6 to 6
- lengths: int32 [8], P('grp'), may hold values from 32 to 512
- norm_gain: float32 [512], replicated, may hold values from 0.1 to 1.9
- out_weight: bfloat16 [512, 1024], replicated, may hold values from -0.25 to 0.25
Outputs:
- layer_out: bfloat16 [4096, 1024], P(('grp', 'blk'))
- grad_query: bfloat16 [4096, 512], P(('grp', 'blk'))
- grad_key: bfloat16 [4096, 512], P(('grp', 'blk'))
- grad_value: bfloat16 [4096, 512], P(('grp', 'blk'))
- grad_gate: bfloat16 [4096, 512], P(('grp', 'blk'))
- grad_weight: float32 [512, 1024], P(None, 'blk')
The draws below stay inside these ranges and needn't reach their ends.
Inputs may be any that keep to these rules, and one draw needn't show every extreme that they name: `lengths`: events of a user at or past its length are padding.
All inputs are finite; a program needn't handle non-finite values.
Results may differ from the reference program's by a relative error of at most 0.009.
Values may be sent and summed in bfloat16 or wider, within the bound.
No kernel may reach another device: no remote copies, remote signals or barrier semaphores. Data moves between devices by JAX's collectives and lax.ppermute only.
A program may use at most 64 MiB of HBM per device.

```python
from functools import partial
import jax
import jax.numpy as jnp
from jax import lax

D = 1024
HEADS = 8
HEAD = 64
HD = 512
NSEQ = 512
USERS = 8
TOKENS = 4096


def plant(result, rng, smallest, high):
    dims = result.shape
    spot = [jax.random.randint(jax.random.fold_in(rng, axis), (), 0, dims[axis]) for axis in range(len(dims))]
    result = result.at[tuple(spot)].set(smallest)
    longest = dims.index(max(dims))
    spot[longest] = (spot[longest] + 1) % dims[longest]
    return result.at[tuple(spot)].set(high)


def with_spikes(result, key, source, target, parts, factor):
    def block_of(position):
        return (jnp.arange(result.shape[position]) // (result.shape[position] // parts)).reshape((-1,) + (1,) * (result.ndim - 1 - position))

    one_side = jax.random.permutation(key, parts)[block_of(target)]
    second = (block_of(target) + parts // 2) % parts
    return jnp.where((block_of(source) == one_side) | (block_of(source) == second), factor * result, result)


def shard_levels(key, shape, shards, low, largest):
    loudness, own = 1.0, jax.random.fold_in(key, 6)
    for dim, parts in shards:
        steps = jnp.exp(jax.random.uniform(jax.random.fold_in(own, dim), (parts,), jnp.float32, low / len(shards), largest / len(shards)))
        loudness = loudness * jnp.repeat(steps, shape[dim] // parts).reshape([-1 if axis == dim else 1 for axis in range(len(shape))])
    return loudness


def gaussian(own_key, shape, spread, bound, cuts=(), kind=jnp.bfloat16):
    factor_of = shard_levels(own_key, shape, cuts, -0.22, 0.18) if cuts else 1.0
    values = jax.random.normal(own_key, shape, jnp.float32) * spread * factor_of
    return jnp.minimum(jnp.maximum(values, -bound), bound).astype(kind)


def heavy_noise(own_key, extent, scale, reach, split, heavy, kind=jnp.bfloat16):
    values = scale * jax.random.normal(own_key, extent, jnp.float32)
    if split:
        values = values * shard_levels(own_key, extent, split, -0.22, 0.18)
    return jnp.clip(with_spikes(values, jax.random.fold_in(own_key, 3), *heavy), -reach, reach).astype(kind)


def setup_inputs(seed: int = 0) -> dict:
    key_of = jax.random.split(jax.random.key(seed), 9)
    query = gaussian(key_of[0], (TOKENS, HD), 1.0, 6.0, ((0, 32),))
    key = gaussian(key_of[1], (TOKENS, HD), 1.0, 6.0, ((0, 32),))
    value = gaussian(key_of[2], (TOKENS, HD), 1.0, 6.0, ((0, 32),))
    gate_u = gaussian(key_of[3], (TOKENS, HD), 1.0, 6.0, ((0, 32),))
    out_grad = heavy_noise(key_of[4], (TOKENS, D), 1.0, 6.0, ((0, 32),), (0, 1, 32, 2.75))
    lengths = plant(jax.random.randint(key_of[5], (USERS,), min(32, NSEQ // 2), NSEQ + 1), jax.random.fold_in(key_of[5], 1), min(32, NSEQ // 2), NSEQ).astype(jnp.int32)
    norm_gain = jnp.clip(1.0 + 0.18 * jax.random.normal(key_of[6], (HD,), jnp.float32), 0.1, 1.9)
    out_weight = gaussian(key_of[7], (HD, D), HD ** -0.5, 0.25)
    return {"query": query, "key": key, "value": value, "gate_u": gate_u, "out_grad": out_grad, "lengths": lengths, "norm_gain": norm_gain, "out_weight": out_weight}


EPS = 1e-05

def user_pass(norm_gain, weight_mat, total, items):
    queries, keys_in, values_in, gates, cotangent, length = items
    count = queries.shape[0]
    scale = HEAD ** (-0.5)
    places = jnp.arange(count, dtype=jnp.int32)
    alive = places < length
    mask = (places[None, :] <= places[:, None]) & alive[:, None] & alive[None, :]
    query_heads = queries.astype(jnp.float32).reshape(count, HEADS, HEAD)
    key_heads = keys_in.astype(jnp.float32).reshape(count, HEADS, HEAD)
    value_heads = values_in.astype(jnp.float32).reshape(count, HEADS, HEAD)
    scores = jnp.einsum('ihd,jhd->hij', query_heads, key_heads) * scale
    weights = (jax.nn.silu(scores) * mask[None]).astype(jnp.bfloat16)
    attended = jnp.einsum('hij,jhd->ihd', weights.astype(jnp.float32), value_heads).reshape(count, HEADS * HEAD)
    centre = attended - lax.optimization_barrier(jnp.mean(attended, axis=1, keepdims=True))
    inv_std = lax.rsqrt(lax.optimization_barrier(jnp.mean(centre * centre, axis=1, keepdims=True)) + EPS)
    normed = centre * inv_std
    scaled = normed * norm_gain
    mixed = (scaled * gates.astype(jnp.float32)).astype(jnp.bfloat16)
    layer_out = jnp.dot(mixed, weight_mat, preferred_element_type=jnp.float32).astype(jnp.bfloat16)
    mixed_grad = jnp.dot(cotangent, weight_mat.T, preferred_element_type=jnp.float32)
    grad_gate = (mixed_grad * scaled).astype(jnp.bfloat16)
    normed_grad = mixed_grad * gates.astype(jnp.float32) * norm_gain
    attended_grad = inv_std * (normed_grad - lax.optimization_barrier(jnp.mean(normed_grad, axis=1, keepdims=True)) - normed * lax.optimization_barrier(jnp.mean(normed_grad * normed, axis=1, keepdims=True)))
    attended_grad = attended_grad.astype(jnp.bfloat16)
    grad_heads = attended_grad.astype(jnp.float32).reshape(count, HEADS, HEAD)
    prob_grad = jnp.einsum('ihd,jhd->hij', grad_heads, value_heads)
    sigma = jax.nn.sigmoid(scores)
    score_grad = (prob_grad * sigma * (1.0 + scores * (1.0 - sigma)) * mask[None]).astype(jnp.bfloat16).astype(jnp.float32)
    grad_query = (jnp.einsum('hij,jhd->ihd', score_grad, key_heads) * scale).reshape(count, HEADS * HEAD).astype(jnp.bfloat16)
    grad_key = (jnp.einsum('hij,ihd->jhd', score_grad, query_heads) * scale).reshape(count, HEADS * HEAD).astype(jnp.bfloat16)
    grad_value = jnp.einsum('hij,ihd->jhd', weights.astype(jnp.float32), grad_heads).reshape(count, HEADS * HEAD).astype(jnp.bfloat16)
    weight_term = jnp.dot(mixed.T, cotangent, preferred_element_type=jnp.float32)
    return (total + weight_term, (layer_out, grad_query, grad_key, grad_value, grad_gate))

def reference(query, key, value, gate_u, out_grad, lengths, norm_gain, out_weight):

    def shaped(array):
        return array.reshape(USERS, NSEQ, array.shape[-1])

    def flatten(array):
        return array.reshape(TOKENS, array.shape[-1])
    start_total = jnp.zeros((HEADS * HEAD, D), jnp.float32)
    stepper = partial(user_pass, norm_gain, out_weight)
    total, results = lax.scan(stepper, start_total, (shaped(query), shaped(key), shaped(value), shaped(gate_u), shaped(out_grad), lengths))
    layer_out, grad_query, grad_key, grad_value, grad_gate = results
    return (flatten(layer_out), flatten(grad_query), flatten(grad_key), flatten(grad_value), flatten(grad_gate), total)
```

```python
import functools

import jax
import jax.numpy as jnp
from jax import lax
from jax.experimental import pallas as pl
from jax.experimental.pallas import tpu as pltpu
from jax.sharding import PartitionSpec as P

HEADS = 8
HEAD = 64
PAIR = 2 * HEAD
EPS = 1e-05
F32 = jnp.float32
BF16 = jnp.bfloat16
CORES = 2

NT = (((1,), (1,)), ((), ()))
NN = (((1,), (0,)), ((), ()))


def dot(a, b, dims=NN):
    return lax.dot_general(a, b, dims, preferred_element_type=F32)


def call(kernel, outs, *args, scalars=0, scratch=(), flops=0):
    smem = pl.BlockSpec(memory_space=pltpu.SMEM)
    vmem = pl.BlockSpec(memory_space=pltpu.VMEM)
    return pl.pallas_call(
        kernel,
        out_shape=[jax.ShapeDtypeStruct(s, d) for s, d in outs],
        in_specs=[smem] * scalars + [vmem] * (len(args) - scalars),
        out_specs=[vmem] * len(outs),
        scratch_shapes=list(scratch),
        cost_estimate=pl.CostEstimate(flops=flops, transcendentals=0, bytes_accessed=0),
    )(*args)


def partner(index, k, size):
    if size & (size - 1) == 0:
        return index ^ k
    return (index + k) % size


def source(index, k, size):
    if size & (size - 1) == 0:
        return index ^ k
    return (index - k) % size if isinstance(index, int) else lax.rem(index - k + size, size)


def target(index, k, size):
    if size & (size - 1) == 0:
        return index ^ k
    return lax.rem(index + k, size)


def swap_core(x, lanes, down=None):
    pairs = [(i, i ^ 1) for i in range(lanes)]
    if down is not None:
        pairs = [(s, d) for s, d in pairs if (d < s) == down]
    return lax.ppermute(x, "blk", pairs)


def over_chips(x, lanes, k, down):
    step = -k * CORES if down else k * CORES
    pairs = [(i, i + step) for i in range(lanes) if 0 <= i + step < lanes]
    return lax.ppermute(x, "blk", pairs)


def digits(groups):
    out, stride = [], 1
    for size in (2, 4):
        if groups // stride > 1 and (groups // stride) % size == 0:
            out.append((stride, size))
            stride *= size
    if groups // stride > 1:
        out.append((stride, groups // stride))
    return out


def over_digit(x, groups, digit, k):
    stride, size = digit
    pairs = []
    for i in range(groups):
        d = (i // stride) % size
        pairs.append((i, i + (partner(d, k, size) - d) * stride))
    return lax.ppermute(x, "grp", pairs)


def digit_of(digit):
    stride, size = digit
    return lax.rem(lax.div(lax.axis_index("grp"), jnp.int32(stride)), jnp.int32(size))


def low_lanes(shape):
    return lax.broadcasted_iota(jnp.int32, shape, 1) < HEAD


def two_heads(x):
    low = low_lanes(x.shape)
    zero = jnp.zeros_like(x)
    return jnp.concatenate([jnp.where(low, x, zero), jnp.where(low, zero, x)], axis=0)


def one_pair(x):
    rows = x.shape[0] // 2
    top, bottom = x[:rows], x[rows:]
    return jnp.where(low_lanes(top.shape), top, bottom)


def store_blocks(dst, refs, lanes, later):
    pos = lax.axis_index("blk")
    rows = refs[0].shape[0]
    chips = lanes // CORES
    chip, core = lax.div(pos, CORES), lax.rem(pos, CORES)
    for n, ref in enumerate(refs):
        step, other = n // 2, n % 2
        move = step if later else chips - step
        block = lax.rem(chip + move, chips) * CORES + lax.rem(core + other, CORES)
        dst[pl.ds(pl.multiple_of(block * rows, rows), rows), :] = ref[...]


def limits(length, shape, rows):
    pos = lax.axis_index("blk")
    local = lax.rem(lax.broadcasted_iota(jnp.int32, shape, 0), rows)
    row = local + pos * rows
    return jnp.where(row < length, row, -1)


def mixed_grad_kernel(og_ref, w_ref, mg_ref):
    mg_ref[...] = dot(og_ref[...], w_ref[...], NT)


def forward_kernel(lanes, *refs):
    count = lanes
    len_ref, q_ref = refs[:2]
    k_refs = refs[2 : 2 + count]
    v_refs = refs[2 + count : 2 + 2 * count]
    gate_ref, gain_ref, mg_ref = refs[2 + 2 * count : 5 + 2 * count]
    mixed_ref, mixed_t_ref, ag_ref, gg_ref, kall, vall = refs[5 + 2 * count : 11 + 2 * count]
    att = refs[-1]
    length = len_ref[0]
    rows, feats = q_ref.shape
    total = kall.shape[0]
    tile = min(total, 512)
    store_blocks(kall, k_refs, lanes, False)
    store_blocks(vall, v_refs, lanes, False)
    limit = limits(length, (2 * rows, tile), rows)
    key = lax.broadcasted_iota(jnp.int32, (2 * rows, tile), 1)
    for p in range(feats // PAIR):
        cols = slice(p * PAIR, (p + 1) * PAIR)
        lhs = two_heads(q_ref[:, cols] * BF16(HEAD ** -0.5 / 2))

        def step(t, acc, lhs=lhs, cols=cols):
            at = pl.ds(pl.multiple_of(t * tile, tile), tile)
            half = dot(lhs, kall[at, cols], NT)
            weight = jnp.where(key + t * tile <= limit, half + half * jnp.tanh(half), 0.0)
            return acc + dot(weight.astype(BF16), vall[at, cols])

        zero = jnp.zeros((2 * rows, PAIR), F32)
        acc = step(0, zero) if total == tile else lax.fori_loop(0, total // tile, step, zero)
        att[:, cols] = one_pair(acc)
    attended = att[...]
    centre = attended - jnp.mean(attended, axis=1, keepdims=True)
    inv_std = lax.rsqrt(jnp.mean(centre * centre, axis=1, keepdims=True) + EPS)
    normed = centre * inv_std
    gain = gain_ref[...]
    scaled = normed * gain
    gates = gate_ref[...].astype(F32)
    mixed = scaled * gates
    mixed_ref[...] = mixed.astype(BF16)
    mixed_t_ref[...] = mixed.T.astype(BF16)
    mixed_grad = mg_ref[...]
    gg_ref[...] = (mixed_grad * scaled).astype(BF16)
    normed_grad = mixed_grad * gates * gain
    grad = inv_std * (
        normed_grad
        - jnp.mean(normed_grad, axis=1, keepdims=True)
        - normed * jnp.mean(normed_grad * normed, axis=1, keepdims=True)
    )
    ag_ref[...] = grad.astype(BF16)


def query_kernel(len_ref, q_ref, kall, vall, ag_ref, mixed_ref, w_ref, lo_ref, dq_ref):
    length = len_ref[0]
    rows, feats = q_ref.shape
    total = kall.shape[0]
    tile = min(total, 512)
    lo_ref[...] = dot(mixed_ref[...], w_ref[...]).astype(BF16)
    limit = limits(length, (2 * rows, tile), rows)
    key = lax.broadcasted_iota(jnp.int32, (2 * rows, tile), 1)
    for p in range(feats // PAIR):
        cols = slice(p * PAIR, (p + 1) * PAIR)
        lhs = two_heads(q_ref[:, cols] * BF16(HEAD ** -0.5 / 2))
        grad = two_heads(ag_ref[:, cols])

        def step(t, acc, lhs=lhs, grad=grad, cols=cols):
            at = pl.ds(pl.multiple_of(t * tile, tile), tile)
            half = dot(lhs, kall[at, cols], NT)
            prob_grad = dot(grad, vall[at, cols], NT)
            th = jnp.tanh(half)
            slope = (0.5 + 0.5 * th) * (1.0 + half * (1.0 - th))
            score_grad = jnp.where(key + t * tile <= limit, prob_grad * slope, 0.0)
            return acc + dot(score_grad.astype(BF16), kall[at, cols])

        zero = jnp.zeros((2 * rows, PAIR), F32)
        acc = step(0, zero) if total == tile else lax.fori_loop(0, total // tile, step, zero)
        dq_ref[:, cols] = (one_pair(acc) * HEAD ** -0.5).astype(BF16)


def key_kernel(lanes, *refs):
    count = lanes
    len_ref, k_ref, v_ref = refs[:3]
    q_refs = refs[3 : 3 + count]
    g_refs = refs[3 + count : 3 + 2 * count]
    dk_ref, dv_ref, qall, gall = refs[3 + 2 * count :]
    length = len_ref[0]
    rows, feats = k_ref.shape
    total = qall.shape[0]
    tile = min(total, 512)
    store_blocks(qall, q_refs, lanes, True)
    store_blocks(gall, g_refs, lanes, True)
    pos = lax.axis_index("blk")
    mine = lax.rem(lax.broadcasted_iota(jnp.int32, (2 * rows, tile), 0), rows) + pos * rows
    query = lax.broadcasted_iota(jnp.int32, (2 * rows, tile), 1)
    for p in range(feats // PAIR):
        cols = slice(p * PAIR, (p + 1) * PAIR)
        lhs = two_heads(k_ref[:, cols] * BF16(HEAD ** -0.5 / 2))
        val = two_heads(v_ref[:, cols])

        def step(t, carry, lhs=lhs, val=val, cols=cols):
            dk, dv = carry
            at = pl.ds(pl.multiple_of(t * tile, tile), tile)
            half = dot(lhs, qall[at, cols], NT)
            prob_grad = dot(val, gall[at, cols], NT)
            where = query + t * tile
            live = (mine <= where) & (where < length)
            th = jnp.tanh(half)
            weight = jnp.where(live, half + half * th, 0.0)
            slope = (0.5 + 0.5 * th) * (1.0 + half * (1.0 - th))
            score_grad = jnp.where(live, prob_grad * slope, 0.0)
            dk = dk + dot(score_grad.astype(BF16), qall[at, cols])
            dv = dv + dot(weight.astype(BF16), gall[at, cols])
            return dk, dv

        zero = jnp.zeros((2 * rows, PAIR), F32)
        carry = (zero, zero)
        carry = step(0, carry) if total == tile else lax.fori_loop(0, total // tile, step, carry)
        dk_ref[:, cols] = (one_pair(carry[0]) * HEAD ** -0.5).astype(BF16)
        dv_ref[:, cols] = one_pair(carry[1]).astype(BF16)


def split(total_ref, digit, keep_ref, send_refs):
    size = 1 + len(send_refs)
    part = keep_ref.shape[0]
    mine = digit_of(digit)
    keep_ref[...] = total_ref[pl.ds(pl.multiple_of(mine * part, part), part), :]
    for k, ref in enumerate(send_refs, 1):
        at = target(mine, k, size)
        ref[...] = total_ref[pl.ds(pl.multiple_of(at * part, part), part), :].astype(BF16)


def product_kernel(lanes, digit, *refs):
    m_refs, o_refs = refs[:lanes], refs[lanes : 2 * lanes]
    outs, acc = refs[2 * lanes : -1], refs[-1]
    acc[...] = sum(dot(m[...], o[...]) for m, o in zip(m_refs, o_refs))
    split(acc, digit, outs[0], outs[1:])


def sum_split_kernel(count, whole, digit, *refs):
    outs, acc = refs[1 + count : -1], refs[-1]
    if whole is None:
        total = refs[0][...]
        for ref in refs[1 : 1 + count]:
            total = total + ref[...].astype(F32)
    else:
        mine, size = digit_of(whole), whole[1]
        rows = refs[0].shape[0]
        for k, ref in enumerate(refs[: 1 + count]):
            at = source(mine, k, size) * rows
            acc[pl.ds(pl.multiple_of(at, rows), rows), :] = ref[...].astype(F32)
        total = acc[:rows, :]
        for k in range(1, size):
            total = total + acc[k * rows : (k + 1) * rows, :]
        acc = acc.at[:rows, :]
    acc[...] = total
    if digit is None:
        outs[0][...] = total.astype(outs[0].dtype)
    else:
        split(acc, digit, outs[0], outs[1:])


def join_kernel(digit, *refs):
    parts, out = refs[:-1], refs[-1]
    size, part = len(parts), parts[0].shape[0]
    mine = digit_of(digit)
    for k, ref in enumerate(parts):
        at = source(mine, k, size)
        out[pl.ds(pl.multiple_of(at * part, part), part), :] = ref[...].astype(out.dtype)


def shards(query, key, value, gate_u, out_grad, lengths, norm_gain, out_weight):
    rows, feats = query.shape
    model = out_grad.shape[1]
    lanes = lax.axis_size("blk")
    groups = lax.axis_size("grp")
    chips = lanes // CORES
    pos = lax.axis_index("blk")
    total = rows * lanes
    width = model // lanes

    def spread(x, later):
        cross = [over_chips(x, lanes, k, later) for k in range(1, chips)]
        pieces = [x, swap_core(x, lanes, later)]
        for c in cross:
            pieces += [c, swap_core(c, lanes)]
        return pieces

    keys = spread(key, False)
    values = spread(value, False)
    columns = [
        lax.dynamic_slice_in_dim(out_grad, target(pos, k, lanes) * width, width, 1)
        for k in range(lanes)
    ]
    blk_pairs = [[(i, partner(i, k, lanes)) for i in range(lanes)] for k in range(lanes)]
    columns = columns[:1] + [lax.ppermute(columns[k], "blk", blk_pairs[k]) for k in range(1, lanes)]
    queries = spread(query, True)

    (mixed_grad,) = call(
        mixed_grad_kernel, [((rows, feats), F32)], out_grad, out_weight, flops=2 * rows * feats * model
    )
    attention_flops = 4 * rows * total * feats
    mixed, mixed_t, att_grad, grad_gate, kall, vall = call(
        functools.partial(forward_kernel, lanes),
        [
            ((rows, feats), BF16),
            ((feats, rows), BF16),
            ((rows, feats), BF16),
            ((rows, feats), BF16),
            ((total, feats), BF16),
            ((total, feats), BF16),
        ],
        lengths,
        query,
        *keys,
        *values,
        gate_u,
        norm_gain.reshape(1, feats),
        mixed_grad,
        scalars=1,
        scratch=[pltpu.VMEM((rows, feats), F32)],
        flops=attention_flops,
    )
    mixes = [mixed_t] + [lax.ppermute(mixed_t, "blk", blk_pairs[k]) for k in range(1, lanes)]
    grads = spread(att_grad, True)

    stages = digits(groups)
    size = feats
    plan = []
    for digit in stages:
        parts = digit[1] if size % (16 * digit[1]) == 0 else 1
        size //= parts
        plan.append((digit, parts, size))

    layer_out, grad_query = call(
        query_kernel,
        [((rows, model), BF16), ((rows, feats), BF16)],
        lengths,
        query,
        kall,
        vall,
        att_grad,
        mixed,
        out_weight,
        scalars=1,
        flops=attention_flops,
    )
    grad_key, grad_value = call(
        functools.partial(key_kernel, lanes),
        [((rows, feats), BF16), ((rows, feats), BF16)],
        lengths,
        key,
        value,
        *queries,
        *grads,
        scalars=1,
        scratch=[pltpu.VMEM((total, feats), BF16), pltpu.VMEM((total, feats), BF16)],
        flops=2 * attention_flops,
    )

    def pieces_of(parts, part):
        return [((part, width), F32)] + [((part, width), BF16)] * (parts - 1)

    held = call(
        functools.partial(product_kernel, lanes, plan[0][0]),
        pieces_of(plan[0][1], plan[0][2]),
        *mixes,
        *columns,
        scratch=[pltpu.VMEM((feats, width), F32)],
        flops=2 * total * feats * width,
    )
    for n, (digit, parts, part) in enumerate(plan):
        if parts > 1:
            received = [over_digit(held[k], groups, digit, k) for k in range(1, parts)]
        else:
            held = [held[0].astype(BF16)]
            received = [over_digit(held[0], groups, digit, k) for k in range(1, digit[1])]
        last = n + 1 == len(plan)
        nxt = None if last else plan[n + 1]
        split_next = not last and nxt[1] > 1
        held = call(
            functools.partial(
                sum_split_kernel,
                len(received),
                None if parts > 1 else digit,
                nxt[0] if split_next else None,
            ),
            [((part, width), BF16 if last else F32)] if not split_next else pieces_of(nxt[1], nxt[2]),
            held[0],
            *received,
            scratch=[pltpu.VMEM((part if parts > 1 else part * digit[1], width), F32)],
        )
    piece = held[0]
    gathers = [entry for entry in plan[::-1] if entry[1] > 1]
    for n, (digit, parts, part) in enumerate(gathers):
        received = [over_digit(piece, groups, digit, k) for k in range(1, parts)]
        (piece,) = call(
            functools.partial(join_kernel, digit),
            [((part * parts, width), F32 if n + 1 == len(gathers) else BF16)],
            piece,
            *received,
        )
    return (layer_out, grad_query, grad_key, grad_value, grad_gate, piece.astype(F32))


def solution(mesh):
    rows = P(("grp", "blk"), None)
    return jax.shard_map(
        shards,
        mesh=mesh,
        in_specs=(rows, rows, rows, rows, rows, P("grp"), P(), P()),
        out_specs=(rows, rows, rows, rows, rows, P(None, "blk")),
        check_vma=False,
    )
```

```python
import functools
import math

import jax
import jax.numpy as jnp
from jax import lax
from jax.experimental import pallas as pl
from jax.experimental.pallas import tpu as pltpu
from jax.sharding import PartitionSpec as P


HEAD = 64
PAIR = 2 * HEAD
EPS = 1e-05
F32 = jnp.float32
BF16 = jnp.bfloat16
CORES = 2
WORK_BYTES = 8 << 20

NT = (((1,), (1,)), ((), ()))
NN = (((1,), (0,)), ((), ()))


def dot(a, b, dims=NN):
    return lax.dot_general(a, b, dims, preferred_element_type=F32)


def nbytes(shape, dtype):
    return math.prod(shape) * jnp.dtype(dtype).itemsize


def call(kernel, outs, *args, scalars=0, scratch=(), flops=0):
    smem = pl.BlockSpec(memory_space=pltpu.SMEM)
    vmem = pl.BlockSpec(memory_space=pltpu.VMEM)
    held = sum(nbytes(x.shape, x.dtype) for x in args) + sum(nbytes(*o) for o in outs)
    held += sum(nbytes(x.shape, x.dtype) for x in scratch)
    return pl.pallas_call(
        kernel,
        out_shape=[jax.ShapeDtypeStruct(s, d) for s, d in outs],
        in_specs=[smem] * scalars + [vmem] * (len(args) - scalars),
        out_specs=[vmem] * len(outs),
        scratch_shapes=list(scratch),
        cost_estimate=pl.CostEstimate(flops=flops, transcendentals=0, bytes_accessed=0),
        compiler_params=pltpu.CompilerParams(vmem_limit_bytes=held + WORK_BYTES),
    )(*args)


def is_pow2(size):
    return size & (size - 1) == 0


def target(index, k, size):
    if is_pow2(size):
        return index ^ k
    return (index + k) % size if isinstance(index, int) else lax.rem(index + k, size)


def source(index, k, size):
    if is_pow2(size):
        return index ^ k
    return (index - k) % size if isinstance(index, int) else lax.rem(index + size - k, size)


def over_blk(x, lanes, step, other):
    chips = lanes // CORES
    pairs = []
    for i in range(lanes):
        chip, core = divmod(i, CORES)
        pairs.append((i, target(chip, step, chips) * CORES + (core + other) % CORES))
    return lax.ppermute(x, "blk", pairs)


def digits(groups):
    out, stride = [], 1
    while groups // stride % 2 == 0:
        out.append((stride, 2))
        stride *= 2
    if groups // stride > 1:
        out.append((stride, groups // stride))
    return out


def over_digit(x, groups, digit, k):
    stride, size = digit
    pairs = []
    for i in range(groups):
        d = (i // stride) % size
        pairs.append((i, i + (target(d, k, size) - d) * stride))
    return lax.ppermute(x, "grp", pairs)


def digit_of(digit):
    stride, size = digit
    return lax.rem(lax.div(lax.axis_index("grp"), jnp.int32(stride)), jnp.int32(size))


def low_lanes(shape):
    return lax.broadcasted_iota(jnp.int32, shape, 1) < HEAD


def two_heads(x):
    low = low_lanes(x.shape)
    zero = jnp.zeros_like(x)
    return jnp.concatenate([jnp.where(low, x, zero), jnp.where(low, zero, x)], axis=0)


def one_pair(x):
    rows = x.shape[0] // 2
    top, bottom = x[:rows], x[rows:]
    return jnp.where(low_lanes(top.shape), top, bottom)


def store_blocks(dst, refs, lanes):
    pos = lax.axis_index("blk")
    rows = refs[0].shape[0]
    chips = lanes // CORES
    chip, core = lax.div(pos, CORES), lax.rem(pos, CORES)
    for n, ref in enumerate(refs):
        step, other = n // CORES, n % CORES
        block = source(chip, step, chips) * CORES + lax.rem(core + other, CORES)
        dst[pl.ds(pl.multiple_of(block * rows, rows), rows), :] = ref[...]


def limits(length, shape, rows):
    pos = lax.axis_index("blk")
    local = lax.rem(lax.broadcasted_iota(jnp.int32, shape, 0), rows)
    row = local + pos * rows
    return jnp.where(row < length, row, -1)


def mixed_grad_kernel(chips, og_ref, w_ref, mg_ref, *cols_refs):
    mg_ref[...] = dot(og_ref[...], w_ref[...], NT)
    chip = lax.div(lax.axis_index("blk"), CORES)
    width = cols_refs[0].shape[1]
    for k, ref in enumerate(cols_refs):
        at = target(chip, k, chips) * width
        ref[...] = og_ref[:, pl.ds(pl.multiple_of(at, width), width)]


def forward_kernel(lanes, *refs):
    count = lanes
    len_ref, q_ref = refs[:2]
    k_refs = refs[2 : 2 + count]
    v_refs = refs[2 + count : 2 + 2 * count]
    gate_ref, gain_ref, mg_ref = refs[2 + 2 * count : 5 + 2 * count]
    mixed_ref, mixed_t_ref, ag_ref, gg_ref, kall, vall = refs[5 + 2 * count : 11 + 2 * count]
    att = refs[-1]
    length = len_ref[0]
    rows, feats = q_ref.shape
    total = kall.shape[0]
    tile = min(total, 512)
    store_blocks(kall, k_refs, lanes)
    store_blocks(vall, v_refs, lanes)
    limit = limits(length, (2 * rows, tile), rows)
    key = lax.broadcasted_iota(jnp.int32, (2 * rows, tile), 1)
    for p in range(feats // PAIR):
        cols = slice(p * PAIR, (p + 1) * PAIR)
        lhs = two_heads(q_ref[:, cols] * BF16(HEAD ** -0.5 / 2))

        def step(t, acc, lhs=lhs, cols=cols):
            at = pl.ds(pl.multiple_of(t * tile, tile), tile)
            half = dot(lhs, kall[at, cols], NT)
            weight = jnp.where(key + t * tile <= limit, half + half * jnp.tanh(half), 0.0)
            return acc + dot(weight.astype(BF16), vall[at, cols])

        zero = jnp.zeros((2 * rows, PAIR), F32)
        acc = step(0, zero) if total == tile else lax.fori_loop(0, total // tile, step, zero)
        att[:, cols] = one_pair(acc)
    attended = att[...]
    centre = attended - jnp.mean(attended, axis=1, keepdims=True)
    inv_std = lax.rsqrt(jnp.mean(centre * centre, axis=1, keepdims=True) + EPS)
    normed = centre * inv_std
    gain = gain_ref[...]
    scaled = normed * gain
    gates = gate_ref[...].astype(F32)
    mixed = scaled * gates
    mixed_ref[...] = mixed.astype(BF16)
    mixed_t_ref[...] = mixed.T.astype(BF16)
    mixed_grad = mg_ref[...]
    gg_ref[...] = (mixed_grad * scaled).astype(BF16)
    normed_grad = mixed_grad * gates * gain
    grad = inv_std * (
        normed_grad
        - jnp.mean(normed_grad, axis=1, keepdims=True)
        - normed * jnp.mean(normed_grad * normed, axis=1, keepdims=True)
    )
    ag_ref[...] = grad.astype(BF16)


def query_kernel(len_ref, q_ref, kall, vall, ag_ref, mixed_ref, w_ref, lo_ref, dq_ref):
    length = len_ref[0]
    rows, feats = q_ref.shape
    total = kall.shape[0]
    tile = min(total, 512)
    lo_ref[...] = dot(mixed_ref[...], w_ref[...]).astype(BF16)
    limit = limits(length, (2 * rows, tile), rows)
    key = lax.broadcasted_iota(jnp.int32, (2 * rows, tile), 1)
    for p in range(feats // PAIR):
        cols = slice(p * PAIR, (p + 1) * PAIR)
        lhs = two_heads(q_ref[:, cols] * BF16(HEAD ** -0.5 / 2))
        grad = two_heads(ag_ref[:, cols])

        def step(t, acc, lhs=lhs, grad=grad, cols=cols):
            at = pl.ds(pl.multiple_of(t * tile, tile), tile)
            half = dot(lhs, kall[at, cols], NT)
            prob_grad = dot(grad, vall[at, cols], NT)
            th = jnp.tanh(half)
            slope = (0.5 + 0.5 * th) * (1.0 + half * (1.0 - th))
            score_grad = jnp.where(key + t * tile <= limit, prob_grad * slope, 0.0)
            return acc + dot(score_grad.astype(BF16), kall[at, cols])

        zero = jnp.zeros((2 * rows, PAIR), F32)
        acc = step(0, zero) if total == tile else lax.fori_loop(0, total // tile, step, zero)
        dq_ref[:, cols] = (one_pair(acc) * HEAD ** -0.5).astype(BF16)


def key_kernel(lanes, *refs):
    count = lanes
    len_ref, k_ref, v_ref = refs[:3]
    q_refs = refs[3 : 3 + count]
    g_refs = refs[3 + count : 3 + 2 * count]
    dk_ref, dv_ref, qall, gall = refs[3 + 2 * count :]
    length = len_ref[0]
    rows, feats = k_ref.shape
    total = qall.shape[0]
    tile = min(total, 512)
    store_blocks(qall, q_refs, lanes)
    store_blocks(gall, g_refs, lanes)
    pos = lax.axis_index("blk")
    mine = lax.rem(lax.broadcasted_iota(jnp.int32, (2 * rows, tile), 0), rows) + pos * rows
    query = lax.broadcasted_iota(jnp.int32, (2 * rows, tile), 1)
    for p in range(feats // PAIR):
        cols = slice(p * PAIR, (p + 1) * PAIR)
        lhs = two_heads(k_ref[:, cols] * BF16(HEAD ** -0.5 / 2))
        val = two_heads(v_ref[:, cols])

        def step(t, carry, lhs=lhs, val=val, cols=cols):
            dk, dv = carry
            at = pl.ds(pl.multiple_of(t * tile, tile), tile)
            half = dot(lhs, qall[at, cols], NT)
            prob_grad = dot(val, gall[at, cols], NT)
            where = query + t * tile
            live = (mine <= where) & (where < length)
            th = jnp.tanh(half)
            weight = jnp.where(live, half + half * th, 0.0)
            slope = (0.5 + 0.5 * th) * (1.0 + half * (1.0 - th))
            score_grad = jnp.where(live, prob_grad * slope, 0.0)
            dk = dk + dot(score_grad.astype(BF16), qall[at, cols])
            dv = dv + dot(weight.astype(BF16), gall[at, cols])
            return dk, dv

        zero = jnp.zeros((2 * rows, PAIR), F32)
        carry = (zero, zero)
        carry = step(0, carry) if total == tile else lax.fori_loop(0, total // tile, step, carry)
        dk_ref[:, cols] = (one_pair(carry[0]) * HEAD ** -0.5).astype(BF16)
        dv_ref[:, cols] = one_pair(carry[1]).astype(BF16)


def split(total_ref, digit, keep_ref, send_refs):
    size = 1 + len(send_refs)
    part = keep_ref.shape[0]
    mine = digit_of(digit)
    keep_ref[...] = total_ref[pl.ds(pl.multiple_of(mine * part, part), part), :]
    for k, ref in enumerate(send_refs, 1):
        at = target(mine, k, size)
        ref[...] = total_ref[pl.ds(pl.multiple_of(at * part, part), part), :].astype(BF16)


def product_kernel(lanes, digit, *refs):
    m_refs, o_refs = refs[:lanes], refs[lanes : 2 * lanes]
    outs, acc = refs[2 * lanes : -1], refs[-1]
    width = acc.shape[1]
    first = lax.rem(lax.axis_index("blk"), CORES) == 0
    total = None
    for n in range(0, lanes, CORES):
        lhs = jnp.concatenate([m[...] for m in m_refs[n : n + CORES]], axis=1)
        rhs = jnp.concatenate([o[...] for o in o_refs[n : n + CORES]], axis=0)
        rhs = jnp.where(first, rhs[:, :width], rhs[:, width:])
        part = dot(lhs, rhs)
        total = part if total is None else total + part
    acc[...] = total
    split(acc, digit, outs[0], outs[1:])


def sum_split_kernel(count, whole, digit, *refs):
    outs, acc = refs[1 + count : -1], refs[-1]
    if whole is None:
        total = refs[0][...]
        for ref in refs[1 : 1 + count]:
            total = total + ref[...].astype(F32)
    else:
        mine, size = digit_of(whole), whole[1]
        rows = refs[0].shape[0]
        for k, ref in enumerate(refs[: 1 + count]):
            at = source(mine, k, size) * rows
            acc[pl.ds(pl.multiple_of(at, rows), rows), :] = ref[...].astype(F32)
        total = acc[:rows, :]
        for k in range(1, size):
            total = total + acc[k * rows : (k + 1) * rows, :]
        acc = acc.at[:rows, :]
    acc[...] = total
    if digit is None:
        outs[0][...] = total.astype(outs[0].dtype)
    else:
        split(acc, digit, outs[0], outs[1:])


def join_kernel(digit, *refs):
    parts, out = refs[:-1], refs[-1]
    size, part = len(parts), parts[0].shape[0]
    mine = digit_of(digit)
    for k, ref in enumerate(parts):
        at = source(mine, k, size)
        out[pl.ds(pl.multiple_of(at * part, part), part), :] = ref[...].astype(out.dtype)


def layer(query, key, value, gate_u, out_grad, lengths, norm_gain, out_weight):
    rows, feats = query.shape
    model = out_grad.shape[1]
    lanes = lax.axis_size("blk")
    groups = lax.axis_size("grp")
    chips = lanes // CORES
    total = rows * lanes
    width = model // lanes
    steps = range(1, chips)

    def cross(x):
        return [over_blk(x, lanes, k, 0) for k in steps]

    def cores(pieces):
        out = []
        for x in pieces:
            out += [x, over_blk(x, lanes, 0, 1)]
        return out

    keys = cores([key] + cross(key))
    values = cores([value] + cross(value))
    mixed_grad, *columns = call(
        functools.partial(mixed_grad_kernel, chips),
        [((rows, feats), F32)] + [((rows, model // chips), BF16)] * chips,
        out_grad,
        out_weight,
        flops=2 * rows * feats * model,
    )
    moved = [over_blk(columns[k], lanes, k, 0) for k in steps]
    columns = cores([columns[0]] + moved)
    queries = cores([query] + cross(query))

    attention_flops = 4 * rows * total * feats
    mixed, mixed_t, att_grad, grad_gate, kall, vall = call(
        functools.partial(forward_kernel, lanes),
        [
            ((rows, feats), BF16),
            ((feats, rows), BF16),
            ((rows, feats), BF16),
            ((rows, feats), BF16),
            ((total, feats), BF16),
            ((total, feats), BF16),
        ],
        lengths,
        query,
        *keys,
        *values,
        gate_u,
        norm_gain.reshape(1, feats),
        mixed_grad,
        scalars=1,
        scratch=[pltpu.VMEM((rows, feats), F32)],
        flops=attention_flops,
    )
    mixes = [mixed_t]
    for n in range(1, lanes):
        mixes.append(over_blk(mixed_t, lanes, n // CORES, n % CORES))
    grads = cores([att_grad] + cross(att_grad))

    stages = digits(groups)
    size = feats
    plan = []
    for n, digit in enumerate(stages):
        parts = digit[1] if n == 0 and size % (16 * digit[1]) == 0 else 1
        size //= parts
        plan.append((digit, parts, size))

    layer_out, grad_query = call(
        query_kernel,
        [((rows, model), BF16), ((rows, feats), BF16)],
        lengths,
        query,
        kall,
        vall,
        att_grad,
        mixed,
        out_weight,
        scalars=1,
        flops=attention_flops,
    )
    grad_key, grad_value = call(
        functools.partial(key_kernel, lanes),
        [((rows, feats), BF16), ((rows, feats), BF16)],
        lengths,
        key,
        value,
        *queries,
        *grads,
        scalars=1,
        scratch=[pltpu.VMEM((total, feats), BF16), pltpu.VMEM((total, feats), BF16)],
        flops=2 * attention_flops,
    )

    def pieces_of(parts, part):
        return [((part, width), F32)] + [((part, width), BF16)] * (parts - 1)

    held = call(
        functools.partial(product_kernel, lanes, plan[0][0]),
        pieces_of(plan[0][1], plan[0][2]),
        *mixes,
        *columns,
        scratch=[pltpu.VMEM((feats, width), F32)],
        flops=2 * total * feats * width,
    )
    for n, (digit, parts, part) in enumerate(plan):
        if parts > 1:
            received = [over_digit(held[k], groups, digit, k) for k in range(1, parts)]
        else:
            held = [held[0].astype(BF16)]
            received = [over_digit(held[0], groups, digit, k) for k in range(1, digit[1])]
        last = n + 1 == len(plan)
        nxt = None if last else plan[n + 1]
        split_next = not last and nxt[1] > 1
        held = call(
            functools.partial(
                sum_split_kernel,
                len(received),
                None if parts > 1 else digit,
                nxt[0] if split_next else None,
            ),
            [((part, width), BF16)] if not split_next else pieces_of(nxt[1], nxt[2]),
            held[0],
            *received,
            scratch=[pltpu.VMEM((part if parts > 1 else part * digit[1], width), F32)],
        )
    piece = held[0]
    gathers = [entry for entry in plan[::-1] if entry[1] > 1]
    for n, (digit, parts, part) in enumerate(gathers):
        received = [over_digit(piece, groups, digit, k) for k in range(1, parts)]
        (piece,) = call(
            functools.partial(join_kernel, digit),
            [((part * parts, width), F32 if n + 1 == len(gathers) else BF16)],
            piece,
            *received,
        )
    return (layer_out, grad_query, grad_key, grad_value, grad_gate, piece.astype(F32))


def solution(mesh):
    rows = P(("grp", "blk"), None)
    return jax.shard_map(
        layer,
        mesh=mesh,
        in_specs=(rows, rows, rows, rows, rows, P("grp"), P(), P()),
        out_specs=(rows, rows, rows, rows, rows, P(None, "blk")),
        check_vma=False,
    )
```

```python
import functools
import math

import jax
import jax.numpy as jnp
from jax import lax
from jax.experimental import pallas as pl
from jax.experimental.pallas import tpu as pltpu
from jax.sharding import PartitionSpec as P


HEAD = 64
PAIR = 2 * HEAD
EPS = 1e-05
F32 = jnp.float32
BF16 = jnp.bfloat16
CORES = 2
WORK_BYTES = 8 << 20

NT = (((1,), (1,)), ((), ()))
NN = (((1,), (0,)), ((), ()))


def dot(a, b, dims=NN):
    return lax.dot_general(a, b, dims, preferred_element_type=F32)


def nbytes(shape, dtype):
    return math.prod(shape) * jnp.dtype(dtype).itemsize


def call(kernel, outs, *args, scalars=0, scratch=(), flops=0):
    smem = pl.BlockSpec(memory_space=pltpu.SMEM)
    vmem = pl.BlockSpec(memory_space=pltpu.VMEM)
    held = sum(nbytes(x.shape, x.dtype) for x in args) + sum(nbytes(*o) for o in outs)
    held += sum(nbytes(x.shape, x.dtype) for x in scratch)
    return pl.pallas_call(
        kernel,
        out_shape=[jax.ShapeDtypeStruct(s, d) for s, d in outs],
        in_specs=[smem] * scalars + [vmem] * (len(args) - scalars),
        out_specs=[vmem] * len(outs),
        scratch_shapes=list(scratch),
        cost_estimate=pl.CostEstimate(flops=flops, transcendentals=0, bytes_accessed=0),
        compiler_params=pltpu.CompilerParams(vmem_limit_bytes=held + WORK_BYTES),
    )(*args)


def is_pow2(size):
    return size & (size - 1) == 0


def target(index, k, size):
    if is_pow2(size):
        return index ^ k
    return (index + k) % size if isinstance(index, int) else lax.rem(index + k, size)


def source(index, k, size):
    if is_pow2(size):
        return index ^ k
    return (index - k) % size if isinstance(index, int) else lax.rem(index + size - k, size)


def over_blk(x, lanes, step, other):
    chips = lanes // CORES
    pairs = []
    for i in range(lanes):
        chip, core = divmod(i, CORES)
        pairs.append((i, target(chip, step, chips) * CORES + (core + other) % CORES))
    return lax.ppermute(x, "blk", pairs)


def digits(groups):
    out, stride = [], 1
    for size in [4] + [2] * groups:
        if groups // stride % size == 0:
            out.append((stride, size))
            stride *= size
    if groups // stride > 1:
        out.append((stride, groups // stride))
    return out


def over_digit(x, groups, digit, k):
    stride, size = digit
    pairs = []
    for i in range(groups):
        d = (i // stride) % size
        pairs.append((i, i + (target(d, k, size) - d) * stride))
    return lax.ppermute(x, "grp", pairs)


def digit_of(digit):
    stride, size = digit
    return lax.rem(lax.div(lax.axis_index("grp"), jnp.int32(stride)), jnp.int32(size))


def low_lanes(shape):
    return lax.broadcasted_iota(jnp.int32, shape, 1) < HEAD


def two_heads(x):
    low = low_lanes(x.shape)
    zero = jnp.zeros_like(x)
    return jnp.concatenate([jnp.where(low, x, zero), jnp.where(low, zero, x)], axis=0)


def one_pair(x):
    rows = x.shape[0] // 2
    top, bottom = x[:rows], x[rows:]
    return jnp.where(low_lanes(top.shape), top, bottom)


def store_blocks(dst, refs, lanes):
    pos = lax.axis_index("blk")
    rows = refs[0].shape[0]
    chips = lanes // CORES
    chip, core = lax.div(pos, CORES), lax.rem(pos, CORES)
    for n, ref in enumerate(refs):
        step, other = n // CORES, n % CORES
        block = source(chip, step, chips) * CORES + lax.rem(core + other, CORES)
        dst[pl.ds(pl.multiple_of(block * rows, rows), rows), :] = ref[...]


def limits(length, shape, rows):
    pos = lax.axis_index("blk")
    local = lax.rem(lax.broadcasted_iota(jnp.int32, shape, 0), rows)
    row = local + pos * rows
    return jnp.where(row < length, row, -1)


def mixed_grad_kernel(chips, og_ref, w_ref, mg_ref, *cols_refs):
    mg_ref[...] = dot(og_ref[...], w_ref[...], NT)
    chip = lax.div(lax.axis_index("blk"), CORES)
    width = cols_refs[0].shape[1]
    for k, ref in enumerate(cols_refs):
        at = target(chip, k, chips) * width
        ref[...] = og_ref[:, pl.ds(pl.multiple_of(at, width), width)]


def forward_kernel(lanes, *refs):
    count = lanes
    len_ref, q_ref = refs[:2]
    k_refs = refs[2 : 2 + count]
    v_refs = refs[2 + count : 2 + 2 * count]
    gate_ref, gain_ref, mg_ref = refs[2 + 2 * count : 5 + 2 * count]
    mixed_ref, mixed_t_ref, ag_ref, gg_ref, kall, vall = refs[5 + 2 * count : 11 + 2 * count]
    att = refs[-1]
    length = len_ref[0]
    rows, feats = q_ref.shape
    total = kall.shape[0]
    tile = min(total, 512)
    store_blocks(kall, k_refs, lanes)
    store_blocks(vall, v_refs, lanes)
    limit = limits(length, (2 * rows, tile), rows)
    key = lax.broadcasted_iota(jnp.int32, (2 * rows, tile), 1)
    for p in range(feats // PAIR):
        cols = slice(p * PAIR, (p + 1) * PAIR)
        lhs = two_heads(q_ref[:, cols] * BF16(HEAD ** -0.5 / 2))

        def step(t, acc, lhs=lhs, cols=cols):
            at = pl.ds(pl.multiple_of(t * tile, tile), tile)
            half = dot(lhs, kall[at, cols], NT)
            weight = jnp.where(key + t * tile <= limit, half + half * jnp.tanh(half), 0.0)
            return acc + dot(weight.astype(BF16), vall[at, cols])

        zero = jnp.zeros((2 * rows, PAIR), F32)
        acc = step(0, zero) if total == tile else lax.fori_loop(0, total // tile, step, zero)
        att[:, cols] = one_pair(acc)
    attended = att[...]
    centre = attended - jnp.mean(attended, axis=1, keepdims=True)
    inv_std = lax.rsqrt(jnp.mean(centre * centre, axis=1, keepdims=True) + EPS)
    normed = centre * inv_std
    gain = gain_ref[...]
    scaled = normed * gain
    gates = gate_ref[...].astype(F32)
    mixed = scaled * gates
    mixed_ref[...] = mixed.astype(BF16)
    mixed_t_ref[...] = mixed.T.astype(BF16)
    mixed_grad = mg_ref[...]
    gg_ref[...] = (mixed_grad * scaled).astype(BF16)
    normed_grad = mixed_grad * gates * gain
    grad = inv_std * (
        normed_grad
        - jnp.mean(normed_grad, axis=1, keepdims=True)
        - normed * jnp.mean(normed_grad * normed, axis=1, keepdims=True)
    )
    ag_ref[:, :feats] = grad.astype(BF16)
    ag_ref[:, feats:] = q_ref[...]


def query_kernel(len_ref, q_ref, kall, vall, ag_ref, mixed_ref, w_ref, lo_ref, dq_ref):
    length = len_ref[0]
    rows, feats = q_ref.shape
    total = kall.shape[0]
    tile = min(total, 512)
    lo_ref[...] = dot(mixed_ref[...], w_ref[...]).astype(BF16)
    limit = limits(length, (2 * rows, tile), rows)
    key = lax.broadcasted_iota(jnp.int32, (2 * rows, tile), 1)
    for p in range(feats // PAIR):
        cols = slice(p * PAIR, (p + 1) * PAIR)
        lhs = two_heads(q_ref[:, cols] * BF16(HEAD ** -0.5 / 2))
        grad = two_heads(ag_ref[:, cols])

        def step(t, acc, lhs=lhs, grad=grad, cols=cols):
            at = pl.ds(pl.multiple_of(t * tile, tile), tile)
            half = dot(lhs, kall[at, cols], NT)
            prob_grad = dot(grad, vall[at, cols], NT)
            th = jnp.tanh(half)
            slope = (0.5 + 0.5 * th) * (1.0 + half * (1.0 - th))
            score_grad = jnp.where(key + t * tile <= limit, prob_grad * slope, 0.0)
            return acc + dot(score_grad.astype(BF16), kall[at, cols])

        zero = jnp.zeros((2 * rows, PAIR), F32)
        acc = step(0, zero) if total == tile else lax.fori_loop(0, total // tile, step, zero)
        dq_ref[:, cols] = (one_pair(acc) * HEAD ** -0.5).astype(BF16)


def key_kernel(lanes, *refs):
    count = lanes
    len_ref, k_ref, v_ref = refs[:3]
    dk_ref, dv_ref, gqall = refs[3 + count :]
    length = len_ref[0]
    rows, feats = k_ref.shape
    total = gqall.shape[0]
    tile = min(total, 512)
    store_blocks(gqall, refs[3 : 3 + count], lanes)
    pos = lax.axis_index("blk")
    mine = lax.rem(lax.broadcasted_iota(jnp.int32, (2 * rows, tile), 0), rows) + pos * rows
    query = lax.broadcasted_iota(jnp.int32, (2 * rows, tile), 1)
    for p in range(feats // PAIR):
        cols = slice(p * PAIR, (p + 1) * PAIR)
        lhs = two_heads(k_ref[:, cols] * BF16(HEAD ** -0.5 / 2))
        val = two_heads(v_ref[:, cols])

        q_cols = slice(feats + p * PAIR, feats + (p + 1) * PAIR)

        def step(t, carry, lhs=lhs, val=val, cols=cols, q_cols=q_cols):
            dk, dv = carry
            at = pl.ds(pl.multiple_of(t * tile, tile), tile)
            half = dot(lhs, gqall[at, q_cols], NT)
            prob_grad = dot(val, gqall[at, cols], NT)
            where = query + t * tile
            live = (mine <= where) & (where < length)
            th = jnp.tanh(half)
            weight = jnp.where(live, half + half * th, 0.0)
            slope = (0.5 + 0.5 * th) * (1.0 + half * (1.0 - th))
            score_grad = jnp.where(live, prob_grad * slope, 0.0)
            dk = dk + dot(score_grad.astype(BF16), gqall[at, q_cols])
            dv = dv + dot(weight.astype(BF16), gqall[at, cols])
            return dk, dv

        zero = jnp.zeros((2 * rows, PAIR), F32)
        carry = (zero, zero)
        carry = step(0, carry) if total == tile else lax.fori_loop(0, total // tile, step, carry)
        dk_ref[:, cols] = (one_pair(carry[0]) * HEAD ** -0.5).astype(BF16)
        dv_ref[:, cols] = one_pair(carry[1]).astype(BF16)


def split(total_ref, digit, keep_ref, send_refs):
    size = 1 + len(send_refs)
    part = keep_ref.shape[0]
    mine = digit_of(digit)
    keep_ref[...] = total_ref[pl.ds(pl.multiple_of(mine * part, part), part), :]
    for k, ref in enumerate(send_refs, 1):
        at = target(mine, k, size)
        ref[...] = total_ref[pl.ds(pl.multiple_of(at * part, part), part), :].astype(BF16)


def product_kernel(lanes, digit, *refs):
    m_refs, o_refs = refs[:lanes], refs[lanes : 2 * lanes]
    outs, acc = refs[2 * lanes : -1], refs[-1]
    width = acc.shape[1]
    first = lax.rem(lax.axis_index("blk"), CORES) == 0
    total = None
    for n in range(0, lanes, CORES):
        lhs = jnp.concatenate([m[...] for m in m_refs[n : n + CORES]], axis=1)
        rhs = jnp.concatenate([o[...] for o in o_refs[n : n + CORES]], axis=0)
        rhs = jnp.where(first, rhs[:, :width], rhs[:, width:])
        part = dot(lhs, rhs)
        total = part if total is None else total + part
    acc[...] = total
    split(acc, digit, outs[0], outs[1:])


def sum_split_kernel(count, whole, digit, *refs):
    outs, acc = refs[1 + count : -1], refs[-1]
    if whole is None:
        total = refs[0][...]
        for ref in refs[1 : 1 + count]:
            total = total + ref[...].astype(F32)
    else:
        mine, size = digit_of(whole), whole[1]
        rows = refs[0].shape[0]
        for k, ref in enumerate(refs[: 1 + count]):
            at = source(mine, k, size) * rows
            acc[pl.ds(pl.multiple_of(at, rows), rows), :] = ref[...].astype(F32)
        total = acc[:rows, :]
        for k in range(1, size):
            total = total + acc[k * rows : (k + 1) * rows, :]
        acc = acc.at[:rows, :]
    acc[...] = total
    if digit is None:
        outs[0][...] = total.astype(outs[0].dtype)
    else:
        split(acc, digit, outs[0], outs[1:])


def join_kernel(digit, *refs):
    parts, out = refs[:-1], refs[-1]
    size, part = len(parts), parts[0].shape[0]
    mine = digit_of(digit)
    for k, ref in enumerate(parts):
        at = source(mine, k, size)
        out[pl.ds(pl.multiple_of(at * part, part), part), :] = ref[...].astype(out.dtype)


def layer(query, key, value, gate_u, out_grad, lengths, norm_gain, out_weight):
    rows, feats = query.shape
    model = out_grad.shape[1]
    lanes = lax.axis_size("blk")
    groups = lax.axis_size("grp")
    chips = lanes // CORES
    total = rows * lanes
    width = model // lanes
    steps = range(1, chips)

    def cross(x):
        return [over_blk(x, lanes, k, 0) for k in steps]

    def cores(pieces):
        out = []
        for x in pieces:
            out += [x, over_blk(x, lanes, 0, 1)]
        return out

    keys = cores([key] + cross(key))
    values = cores([value] + cross(value))
    mixed_grad, *columns = call(
        functools.partial(mixed_grad_kernel, chips),
        [((rows, feats), F32)] + [((rows, model // chips), BF16)] * chips,
        out_grad,
        out_weight,
        flops=2 * rows * feats * model,
    )
    moved = [over_blk(columns[k], lanes, k, 0) for k in steps]
    columns = cores([columns[0]] + moved)

    attention_flops = 4 * rows * total * feats
    mixed, mixed_t, grads_queries, grad_gate, kall, vall = call(
        functools.partial(forward_kernel, lanes),
        [
            ((rows, feats), BF16),
            ((feats, rows), BF16),
            ((rows, 2 * feats), BF16),
            ((rows, feats), BF16),
            ((total, feats), BF16),
            ((total, feats), BF16),
        ],
        lengths,
        query,
        *keys,
        *values,
        gate_u,
        norm_gain.reshape(1, feats),
        mixed_grad,
        scalars=1,
        scratch=[pltpu.VMEM((rows, feats), F32)],
        flops=attention_flops,
    )
    mixes = cores([mixed_t] + cross(mixed_t))
    grads = cores([grads_queries] + cross(grads_queries))

    stages = digits(groups)
    size = feats
    plan = []
    for n, digit in enumerate(stages):
        parts = digit[1] if n == 0 and size % (16 * digit[1]) == 0 else 1
        size //= parts
        plan.append((digit, parts, size))

    layer_out, grad_query = call(
        query_kernel,
        [((rows, model), BF16), ((rows, feats), BF16)],
        lengths,
        query,
        kall,
        vall,
        grads_queries,
        mixed,
        out_weight,
        scalars=1,
        flops=attention_flops,
    )
    grad_key, grad_value = call(
        functools.partial(key_kernel, lanes),
        [((rows, feats), BF16), ((rows, feats), BF16)],
        lengths,
        key,
        value,
        *grads,
        scalars=1,
        scratch=[pltpu.VMEM((total, 2 * feats), BF16)],
        flops=2 * attention_flops,
    )

    def pieces_of(parts, part):
        return [((part, width), F32)] + [((part, width), BF16)] * (parts - 1)

    held = call(
        functools.partial(product_kernel, lanes, plan[0][0]),
        pieces_of(plan[0][1], plan[0][2]),
        *mixes,
        *columns,
        scratch=[pltpu.VMEM((feats, width), F32)],
        flops=2 * total * feats * width,
    )
    for n, (digit, parts, part) in enumerate(plan):
        if parts > 1:
            received = [over_digit(held[k], groups, digit, k) for k in range(1, parts)]
        else:
            held = [held[0].astype(BF16)]
            received = [over_digit(held[0], groups, digit, k) for k in range(1, digit[1])]
        last = n + 1 == len(plan)
        nxt = None if last else plan[n + 1]
        split_next = not last and nxt[1] > 1
        held = call(
            functools.partial(
                sum_split_kernel,
                len(received),
                None if parts > 1 else digit,
                nxt[0] if split_next else None,
            ),
            [((part, width), BF16)] if not split_next else pieces_of(nxt[1], nxt[2]),
            held[0],
            *received,
            scratch=[pltpu.VMEM((part if parts > 1 else part * digit[1], width), F32)],
        )
    piece = held[0]
    gathers = [entry for entry in plan[::-1] if entry[1] > 1]
    for n, (digit, parts, part) in enumerate(gathers):
        received = [over_digit(piece, groups, digit, k) for k in range(1, parts)]
        (piece,) = call(
            functools.partial(join_kernel, digit),
            [((part * parts, width), F32 if n + 1 == len(gathers) else BF16)],
            piece,
            *received,
        )
    return (layer_out, grad_query, grad_key, grad_value, grad_gate, piece.astype(F32))


def solution(mesh):
    rows = P(("grp", "blk"), None)
    return jax.shard_map(
        layer,
        mesh=mesh,
        in_specs=(rows, rows, rows, rows, rows, P("grp"), P(), P()),
        out_specs=(rows, rows, rows, rows, rows, P(None, "blk")),
        check_vma=False,
    )
```

```python
import functools
import math

import jax
import jax.numpy as jnp
from jax import lax
from jax.experimental import pallas as pl
from jax.experimental.pallas import tpu as pltpu
from jax.sharding import PartitionSpec as P


HEAD = 64
PAIR = 2 * HEAD
EPS = 1e-05
F32 = jnp.float32
BF16 = jnp.bfloat16
CORES = 2
WORK_BYTES = 8 << 20

NT = (((1,), (1,)), ((), ()))
NN = (((1,), (0,)), ((), ()))


def dot(a, b, dims=NN):
    return lax.dot_general(a, b, dims, preferred_element_type=F32)


def nbytes(shape, dtype):
    return math.prod(shape) * jnp.dtype(dtype).itemsize


def call(kernel, outs, *args, scalars=0, scratch=(), flops=0, space=pltpu.VMEM):
    smem = pl.BlockSpec(memory_space=pltpu.SMEM)
    vmem = pl.BlockSpec(memory_space=pltpu.VMEM)
    inputs = pl.BlockSpec(memory_space=space)
    held = sum(nbytes(x.shape, x.dtype) for x in args) + sum(nbytes(*o) for o in outs)
    held += sum(nbytes(x.shape, x.dtype) for x in scratch if x.memory_space == pltpu.VMEM)
    return pl.pallas_call(
        kernel,
        out_shape=[jax.ShapeDtypeStruct(s, d) for s, d in outs],
        in_specs=[smem] * scalars + [inputs] * (len(args) - scalars),
        out_specs=[vmem] * len(outs),
        scratch_shapes=list(scratch),
        cost_estimate=pl.CostEstimate(flops=flops, transcendentals=0, bytes_accessed=0),
        compiler_params=pltpu.CompilerParams(vmem_limit_bytes=held + WORK_BYTES),
    )(*args)


def is_pow2(size):
    return size & (size - 1) == 0


def target(index, k, size):
    if is_pow2(size):
        return index ^ k
    return (index + k) % size if isinstance(index, int) else lax.rem(index + k, size)


def source(index, k, size):
    if is_pow2(size):
        return index ^ k
    return (index - k) % size if isinstance(index, int) else lax.rem(index + size - k, size)


def over_blk(x, lanes, step, other):
    chips = lanes // CORES
    pairs = []
    for i in range(lanes):
        chip, core = divmod(i, CORES)
        pairs.append((i, target(chip, step, chips) * CORES + (core + other) % CORES))
    return lax.ppermute(x, "blk", pairs)


def digits(groups):
    out, stride = [], 1
    for size in [4] + [2] * groups:
        if groups // stride % size == 0:
            out.append((stride, size))
            stride *= size
    if groups // stride > 1:
        out.append((stride, groups // stride))
    return out


def over_digit(x, groups, digit, k):
    stride, size = digit
    pairs = []
    for i in range(groups):
        d = (i // stride) % size
        pairs.append((i, i + (target(d, k, size) - d) * stride))
    return lax.ppermute(x, "grp", pairs)


def digit_of(digit):
    stride, size = digit
    return lax.rem(lax.div(lax.axis_index("grp"), jnp.int32(stride)), jnp.int32(size))


def low_lanes(shape):
    return lax.broadcasted_iota(jnp.int32, shape, 1) < HEAD


def two_heads(x):
    low = low_lanes(x.shape)
    zero = jnp.zeros_like(x)
    return jnp.concatenate([jnp.where(low, x, zero), jnp.where(low, zero, x)], axis=0)


def one_pair(x):
    rows = x.shape[0] // 2
    top, bottom = x[:rows], x[rows:]
    return jnp.where(low_lanes(top.shape), top, bottom)


def block_at(n, lanes):
    chips = lanes // CORES
    pos = lax.axis_index("blk")
    chip, core = lax.div(pos, CORES), lax.rem(pos, CORES)
    return source(chip, n // CORES, chips) * CORES + lax.rem(core + n % CORES, CORES)


def tiles(blocks, size=4):
    return [blocks[n : n + size] for n in range(0, len(blocks), size)]


def places(blocks, lanes, rows):
    lane = lax.broadcasted_iota(jnp.int32, (1, rows), 1)
    return jnp.concatenate([block_at(n, lanes) * rows + lane for n in blocks], axis=1)


def limits(length, rows):
    pos = lax.axis_index("blk")
    local = lax.rem(lax.broadcasted_iota(jnp.int32, (CORES * rows, 1), 0), rows)
    row = local + pos * rows
    return jnp.where(row < length, row, -1)


def stack(refs, blocks, cols):
    return jnp.concatenate([refs[n][:, cols] for n in blocks], axis=0)


def pair_slices(feats):
    return [slice(p * PAIR, (p + 1) * PAIR) for p in range(feats // PAIR)]


HALF_SCALE = HEAD ** -0.5 / 2


def fetch_kernel(chips, og_ref, *refs):
    count = (len(refs) - chips - 1) // 2
    sources, outs, sem = list(refs[:count]), refs[count:-1], refs[-1]
    chip = lax.div(lax.axis_index("blk"), CORES)
    width = outs[-1].shape[1]
    for k in range(chips):
        at = pl.multiple_of(target(chip, k, chips) * width, width)
        sources.append(og_ref.at[:, pl.ds(at, width)])
    copies = [
        pltpu.make_async_copy(src, dst, sem.at[n]) for n, (src, dst) in enumerate(zip(sources, outs))
    ]
    for copy in copies:
        copy.start()
    for copy in copies:
        copy.wait()


def attend(lanes, length, q_ref, k_refs, v_refs, blocks, cols):
    rows = q_ref.shape[0]
    lhs = two_heads(q_ref[:, cols] * BF16(HALF_SCALE))
    limit = limits(length, rows)
    acc = None
    for some in tiles(blocks):
        half = dot(lhs, stack(k_refs, some, cols), NT)
        live = places(some, lanes, rows) <= limit
        weight = jnp.where(live, half + half * jnp.tanh(half), 0.0).astype(BF16)
        part = dot(weight, stack(v_refs, some, cols))
        acc = part if acc is None else acc + part
    return one_pair(acc)


def partial_kernel(lanes, blocks, *refs):
    len_ref, q_ref = refs[:2]
    k_refs = dict(zip(blocks, refs[2 : 2 + len(blocks)]))
    v_refs = dict(zip(blocks, refs[2 + len(blocks) :]))
    before, out_ref = refs[2 + 2 * len(blocks) : -1], refs[-1]
    length = len_ref[0]
    for cols in pair_slices(q_ref.shape[1]):
        part = attend(lanes, length, q_ref, k_refs, v_refs, blocks, cols)
        for ref in before:
            part = part + ref[:, cols]
        out_ref[:, cols] = part


def forward_kernel(lanes, blocks, *refs):
    len_ref, q_ref = refs[:2]
    count = len(blocks)
    k_refs = dict(zip(blocks, refs[2 : 2 + count]))
    v_refs = dict(zip(blocks, refs[2 + count :]))
    near_ref, gate_ref, gain_ref = refs[2 + 2 * count : 5 + 2 * count]
    mixed_ref, mixed_t_ref, normed_ref, inv_ref, att = refs[5 + 2 * count :]
    length = len_ref[0]
    for cols in pair_slices(q_ref.shape[1]):
        att[:, cols] = near_ref[:, cols] + attend(
            lanes, length, q_ref, k_refs, v_refs, blocks, cols
        )
    attended = att[...]
    centre = attended - jnp.mean(attended, axis=1, keepdims=True)
    inv_std = lax.rsqrt(jnp.mean(centre * centre, axis=1, keepdims=True) + EPS)
    normed = centre * inv_std
    mixed = (normed * gain_ref[...] * gate_ref[...].astype(F32)).astype(BF16)
    mixed_t_ref[...] = mixed.T
    mixed_ref[...] = mixed
    normed_ref[...] = normed
    inv_ref[...] = jnp.broadcast_to(inv_std, inv_ref.shape)


def query_kernel(lanes, *refs):
    len_ref, q_ref = refs[:2]
    k_refs, v_refs = refs[2 : 2 + lanes], refs[2 + lanes : 2 + 2 * lanes]
    gate_ref, gain_ref, og_ref, normed_ref, inv_ref, mixed_ref, w_ref = refs[2 + 2 * lanes : 9 + 2 * lanes]
    lo_ref, dq_ref, gg_ref, gq_ref = refs[9 + 2 * lanes :]
    length = len_ref[0]
    rows, feats = q_ref.shape
    gain = gain_ref[...]
    normed = normed_ref[...]
    mixed_grad = dot(og_ref[...], w_ref[...], NT)
    gg_ref[...] = (mixed_grad * (normed * gain)).astype(BF16)
    normed_grad = mixed_grad * gate_ref[...].astype(F32) * gain
    grad = inv_ref[:, :1] * (
        normed_grad
        - jnp.mean(normed_grad, axis=1, keepdims=True)
        - normed * jnp.mean(normed_grad * normed, axis=1, keepdims=True)
    )
    gq_ref[:, :feats] = grad.astype(BF16)
    gq_ref[:, feats:] = q_ref[...]
    lo_ref[...] = dot(mixed_ref[...], w_ref[...]).astype(BF16)
    limit = limits(length, rows)
    for cols in pair_slices(feats):
        lhs = two_heads(q_ref[:, cols] * BF16(HALF_SCALE))
        grads = two_heads(gq_ref[:, cols])
        acc = None
        for blocks in tiles(range(lanes)):
            keys = stack(k_refs, blocks, cols)
            half = dot(lhs, keys, NT)
            prob_grad = dot(grads, stack(v_refs, blocks, cols), NT)
            th = jnp.tanh(half)
            slope = (0.5 + 0.5 * th) * (1.0 + half * (1.0 - th))
            live = places(blocks, lanes, rows) <= limit
            score_grad = jnp.where(live, prob_grad * slope, 0.0).astype(BF16)
            part = dot(score_grad, keys)
            acc = part if acc is None else acc + part
        dq_ref[:, cols] = (one_pair(acc) * HEAD ** -0.5).astype(BF16)


def key_kernel(lanes, *refs):
    len_ref, k_ref, v_ref = refs[:3]
    gq_refs = refs[3 : 3 + lanes]
    dk_ref, dv_ref = refs[3 + lanes :]
    length = len_ref[0]
    rows, feats = k_ref.shape
    pos = lax.axis_index("blk")
    mine = lax.rem(lax.broadcasted_iota(jnp.int32, (CORES * rows, 1), 0), rows) + pos * rows
    for p, cols in enumerate(pair_slices(feats)):
        lhs = two_heads(k_ref[:, cols] * BF16(HALF_SCALE))
        val = two_heads(v_ref[:, cols])
        q_cols = slice(feats + p * PAIR, feats + (p + 1) * PAIR)
        dk = dv = None
        for blocks in tiles(range(lanes)):
            queries = stack(gq_refs, blocks, q_cols)
            grads = stack(gq_refs, blocks, cols)
            half = dot(lhs, queries, NT)
            prob_grad = dot(val, grads, NT)
            where = places(blocks, lanes, rows)
            where = jnp.where(where < length, where, -1)
            live = mine <= where
            th = jnp.tanh(half)
            weight = jnp.where(live, half + half * th, 0.0).astype(BF16)
            slope = (0.5 + 0.5 * th) * (1.0 + half * (1.0 - th))
            score_grad = jnp.where(live, prob_grad * slope, 0.0).astype(BF16)
            part_k, part_v = dot(score_grad, queries), dot(weight, grads)
            dk = part_k if dk is None else dk + part_k
            dv = part_v if dv is None else dv + part_v
        dk_ref[:, cols] = (one_pair(dk) * HEAD ** -0.5).astype(BF16)
        dv_ref[:, cols] = one_pair(dv).astype(BF16)


def split(total_ref, digit, keep_ref, send_refs):
    size = 1 + len(send_refs)
    part = keep_ref.shape[0]
    mine = digit_of(digit)
    keep_ref[...] = total_ref[pl.ds(pl.multiple_of(mine * part, part), part), :]
    for k, ref in enumerate(send_refs, 1):
        at = target(mine, k, size)
        ref[...] = total_ref[pl.ds(pl.multiple_of(at * part, part), part), :].astype(BF16)


def product_kernel(lanes, digit, *refs):
    m_refs, o_refs = refs[:lanes], refs[lanes : 2 * lanes]
    outs, acc = refs[2 * lanes : -1], refs[-1]
    width = acc.shape[1]
    first = lax.rem(lax.axis_index("blk"), CORES) == 0
    total = None
    for n in range(0, lanes, CORES):
        lhs = jnp.concatenate([m[...] for m in m_refs[n : n + CORES]], axis=1)
        rhs = jnp.concatenate([o[...] for o in o_refs[n : n + CORES]], axis=0)
        rhs = jnp.where(first, rhs[:, :width], rhs[:, width:])
        part = dot(lhs, rhs)
        total = part if total is None else total + part
    acc[...] = total
    split(acc, digit, outs[0], outs[1:])


def sum_split_kernel(count, whole, digit, *refs):
    outs, acc = refs[1 + count : -1], refs[-1]
    if whole is None:
        total = refs[0][...]
        for ref in refs[1 : 1 + count]:
            total = total + ref[...].astype(F32)
    else:
        mine, size = digit_of(whole), whole[1]
        rows = refs[0].shape[0]
        for k, ref in enumerate(refs[: 1 + count]):
            at = source(mine, k, size) * rows
            acc[pl.ds(pl.multiple_of(at, rows), rows), :] = ref[...].astype(F32)
        total = acc[:rows, :]
        for k in range(1, size):
            total = total + acc[k * rows : (k + 1) * rows, :]
        acc = acc.at[:rows, :]
    acc[...] = total
    if digit is None:
        outs[0][...] = total.astype(outs[0].dtype)
    else:
        split(acc, digit, outs[0], outs[1:])


def join_kernel(digit, *refs):
    parts, out = refs[:-1], refs[-1]
    size, part = len(parts), parts[0].shape[0]
    mine = digit_of(digit)
    for k, ref in enumerate(parts):
        at = source(mine, k, size)
        out[pl.ds(pl.multiple_of(at * part, part), part), :] = ref[...].astype(out.dtype)


def layer(query, key, value, gate_u, out_grad, lengths, norm_gain, out_weight):
    rows, feats = query.shape
    model = out_grad.shape[1]
    lanes = lax.axis_size("blk")
    groups = lax.axis_size("grp")
    chips = lanes // CORES
    total = rows * lanes
    width = model // lanes
    steps = range(1, chips)

    def cross(x):
        return [over_blk(x, lanes, k, 0) for k in steps]

    def cores(pieces):
        out = []
        for x in pieces:
            out += [x, over_blk(x, lanes, 0, 1)]
        return out

    keys = cores([key] + cross(key))
    values = cores([value] + cross(value))
    query_here, key_here, value_here, gates, *columns = call(
        functools.partial(fetch_kernel, chips),
        [((rows, feats), BF16)] * 4 + [((rows, model // chips), BF16)] * chips,
        *(pltpu.with_memory_space_constraint(x, pltpu.HBM) for x in (out_grad, query, key, value, gate_u)),
        scratch=[pltpu.SemaphoreType.DMA((4 + chips,))],
        space=pltpu.HBM,
    )
    keys[0], values[0] = key_here, value_here
    moved = [over_blk(columns[k], lanes, k, 0) for k in steps]
    columns = cores([columns[0]] + moved)

    attention_flops = 4 * rows * total * feats
    gain = norm_gain.reshape(1, feats)

    def share(blocks, *before):
        return call(
            functools.partial(partial_kernel, lanes, blocks),
            [((rows, feats), F32)],
            lengths,
            query_here,
            *(keys[n] for n in blocks),
            *(values[n] for n in blocks),
            *before,
            scalars=1,
            flops=attention_flops * len(blocks) // lanes,
        )

    attended = share(list(range(CORES)))
    last = list(range(CORES + 1, lanes, CORES))
    if last:
        attended = share(list(range(CORES, lanes, CORES)), *attended)
    mixed, mixed_t, normed, inv_std = call(
        functools.partial(forward_kernel, lanes, last),
        [
            ((rows, feats), BF16),
            ((feats, rows), BF16),
            ((rows, feats), F32),
            ((rows, PAIR), F32),
        ],
        lengths,
        query_here,
        *(keys[n] for n in last),
        *(values[n] for n in last),
        *attended,
        gates,
        gain,
        scalars=1,
        scratch=[pltpu.VMEM((rows, feats), F32)],
        flops=attention_flops * len(last) // lanes,
    )
    mixes = cores([mixed_t] + cross(mixed_t))
    layer_out, grad_query, grad_gate, grads_queries = call(
        functools.partial(query_kernel, lanes),
        [
            ((rows, model), BF16),
            ((rows, feats), BF16),
            ((rows, feats), BF16),
            ((rows, 2 * feats), BF16),
        ],
        lengths,
        query_here,
        *keys,
        *values,
        gates,
        gain,
        out_grad,
        normed,
        inv_std,
        mixed,
        out_weight,
        scalars=1,
        flops=attention_flops + 4 * rows * feats * model,
    )
    grads = cores([grads_queries] + cross(grads_queries))
    grad_key, grad_value = call(
        functools.partial(key_kernel, lanes),
        [((rows, feats), BF16), ((rows, feats), BF16)],
        lengths,
        key_here,
        value_here,
        *grads,
        scalars=1,
        flops=2 * attention_flops,
    )

    stages = digits(groups)
    size = feats
    plan = []
    for n, digit in enumerate(stages):
        parts = digit[1] if n == 0 and size % (16 * digit[1]) == 0 else 1
        size //= parts
        plan.append((digit, parts, size))

    def pieces_of(parts, part):
        return [((part, width), F32)] + [((part, width), BF16)] * (parts - 1)

    held = call(
        functools.partial(product_kernel, lanes, plan[0][0]),
        pieces_of(plan[0][1], plan[0][2]),
        *mixes,
        *columns,
        scratch=[pltpu.VMEM((feats, width), F32)],
        flops=2 * total * feats * width,
    )
    for n, (digit, parts, part) in enumerate(plan):
        if parts > 1:
            received = [over_digit(held[k], groups, digit, k) for k in range(1, parts)]
        else:
            held = [held[0].astype(BF16)]
            received = [over_digit(held[0], groups, digit, k) for k in range(1, digit[1])]
        last = n + 1 == len(plan)
        nxt = None if last else plan[n + 1]
        split_next = not last and nxt[1] > 1
        held = call(
            functools.partial(
                sum_split_kernel,
                len(received),
                None if parts > 1 else digit,
                nxt[0] if split_next else None,
            ),
            [((part, width), BF16)] if not split_next else pieces_of(nxt[1], nxt[2]),
            held[0],
            *received,
            scratch=[pltpu.VMEM((part if parts > 1 else part * digit[1], width), F32)],
        )
    piece = held[0]
    gathers = [entry for entry in plan[::-1] if entry[1] > 1]
    for n, (digit, parts, part) in enumerate(gathers):
        received = [over_digit(piece, groups, digit, k) for k in range(1, parts)]
        (piece,) = call(
            functools.partial(join_kernel, digit),
            [((part * parts, width), F32 if n + 1 == len(gathers) else BF16)],
            piece,
            *received,
        )
    return (layer_out, grad_query, grad_key, grad_value, grad_gate, piece.astype(F32))


def solution(mesh):
    rows = P(("grp", "blk"), None)
    return jax.shard_map(
        layer,
        mesh=mesh,
        in_specs=(rows, rows, rows, rows, rows, P("grp"), P(), P()),
        out_specs=(rows, rows, rows, rows, rows, P(None, "blk")),
        check_vma=False,
    )
```

```python
import functools
import math

import jax
import jax.numpy as jnp
from jax import lax
from jax.experimental import pallas as pl
from jax.experimental.pallas import tpu as pltpu
from jax.sharding import PartitionSpec as P


HEAD = 64
PAIR = 2 * HEAD
EPS = 1e-05
F32 = jnp.float32
BF16 = jnp.bfloat16
CORES = 2
WORK_BYTES = 8 << 20

NT = (((1,), (1,)), ((), ()))
NN = (((1,), (0,)), ((), ()))


def dot(a, b, dims=NN):
    return lax.dot_general(a, b, dims, preferred_element_type=F32)


def nbytes(shape, dtype):
    return math.prod(shape) * jnp.dtype(dtype).itemsize


def call(kernel, outs, *args, scalars=0, scratch=(), flops=0, space=pltpu.VMEM):
    smem = pl.BlockSpec(memory_space=pltpu.SMEM)
    vmem = pl.BlockSpec(memory_space=pltpu.VMEM)
    inputs = pl.BlockSpec(memory_space=space)
    held = sum(nbytes(x.shape, x.dtype) for x in args) + sum(nbytes(*o) for o in outs)
    held += sum(nbytes(x.shape, x.dtype) for x in scratch if x.memory_space == pltpu.VMEM)
    return pl.pallas_call(
        kernel,
        out_shape=[jax.ShapeDtypeStruct(s, d) for s, d in outs],
        in_specs=[smem] * scalars + [inputs] * (len(args) - scalars),
        out_specs=[vmem] * len(outs),
        scratch_shapes=list(scratch),
        cost_estimate=pl.CostEstimate(flops=flops, transcendentals=0, bytes_accessed=0),
        compiler_params=pltpu.CompilerParams(vmem_limit_bytes=held + WORK_BYTES),
    )(*args)


def is_pow2(size):
    return size & (size - 1) == 0


def target(index, k, size):
    if is_pow2(size):
        return index ^ k
    return (index + k) % size if isinstance(index, int) else lax.rem(index + k, size)


def source(index, k, size):
    if is_pow2(size):
        return index ^ k
    return (index - k) % size if isinstance(index, int) else lax.rem(index + size - k, size)


def over_blk(x, lanes, step, other):
    chips = lanes // CORES
    pairs = []
    for i in range(lanes):
        chip, core = divmod(i, CORES)
        pairs.append((i, target(chip, step, chips) * CORES + (core + other) % CORES))
    return lax.ppermute(x, "blk", pairs)


def digits(groups):
    out, stride = [], 1
    for size in [4] + [2] * groups:
        if groups // stride % size == 0:
            out.append((stride, size))
            stride *= size
    if groups // stride > 1:
        out.append((stride, groups // stride))
    return out


def over_digit(x, groups, digit, k):
    stride, size = digit
    pairs = []
    for i in range(groups):
        d = (i // stride) % size
        pairs.append((i, i + (target(d, k, size) - d) * stride))
    return lax.ppermute(x, "grp", pairs)


def digit_of(digit):
    stride, size = digit
    return lax.rem(lax.div(lax.axis_index("grp"), jnp.int32(stride)), jnp.int32(size))


def low_lanes(shape):
    return lax.broadcasted_iota(jnp.int32, shape, 1) < HEAD


def two_heads(x):
    low = low_lanes(x.shape)
    zero = jnp.zeros_like(x)
    return jnp.concatenate([jnp.where(low, x, zero), jnp.where(low, zero, x)], axis=0)


def one_pair(x):
    rows = x.shape[0] // 2
    top, bottom = x[:rows], x[rows:]
    return jnp.where(low_lanes(top.shape), top, bottom)


def block_at(n, lanes):
    chips = lanes // CORES
    pos = lax.axis_index("blk")
    chip, core = lax.div(pos, CORES), lax.rem(pos, CORES)
    return source(chip, n // CORES, chips) * CORES + lax.rem(core + n % CORES, CORES)


def tiles(blocks, size=4):
    return [blocks[n : n + size] for n in range(0, len(blocks), size)]


def places(blocks, lanes, rows):
    lane = lax.broadcasted_iota(jnp.int32, (1, rows), 1)
    return jnp.concatenate([block_at(n, lanes) * rows + lane for n in blocks], axis=1)


def limits(length, rows):
    pos = lax.axis_index("blk")
    local = lax.rem(lax.broadcasted_iota(jnp.int32, (CORES * rows, 1), 0), rows)
    row = local + pos * rows
    return jnp.where(row < length, row, -1)


def stack(refs, blocks, cols):
    return jnp.concatenate([refs[n][:, cols] for n in blocks], axis=0)


def pair_slices(feats):
    return [slice(p * PAIR, (p + 1) * PAIR) for p in range(feats // PAIR)]


HALF_SCALE = HEAD ** -0.5 / 2


def fetch_kernel(chips, og_ref, *refs):
    count = (len(refs) - chips - 1) // 2
    sources, outs, sem = list(refs[:count]), refs[count:-1], refs[-1]
    chip = lax.div(lax.axis_index("blk"), CORES)
    width = outs[-1].shape[1]
    for k in range(chips):
        at = pl.multiple_of(target(chip, k, chips) * width, width)
        sources.append(og_ref.at[:, pl.ds(at, width)])
    copies = [
        pltpu.make_async_copy(src, dst, sem.at[n]) for n, (src, dst) in enumerate(zip(sources, outs))
    ]
    for copy in copies:
        copy.start()
    for copy in copies:
        copy.wait()


def weight_and_slope(half, live):
    u = jnp.where(live, 1.0 + jnp.tanh(half), 0.0)
    weight = half * u
    return weight, u + weight * (2.0 - u)


def attend(lanes, length, q_ref, k_refs, v_refs, blocks, cols):
    rows = q_ref.shape[0]
    lhs = two_heads(q_ref[:, cols] * BF16(HALF_SCALE))
    limit = limits(length, rows)
    acc = None
    for some in tiles(blocks):
        half = dot(lhs, stack(k_refs, some, cols), NT)
        live = places(some, lanes, rows) <= limit
        weight = jnp.where(live, half + half * jnp.tanh(half), 0.0).astype(BF16)
        part = dot(weight, stack(v_refs, some, cols))
        acc = part if acc is None else acc + part
    return one_pair(acc)


def partial_kernel(lanes, blocks, *refs):
    len_ref, q_ref = refs[:2]
    k_refs = dict(zip(blocks, refs[2 : 2 + len(blocks)]))
    v_refs = dict(zip(blocks, refs[2 + len(blocks) :]))
    before, out_ref = refs[2 + 2 * len(blocks) : -1], refs[-1]
    length = len_ref[0]
    for cols in pair_slices(q_ref.shape[1]):
        part = attend(lanes, length, q_ref, k_refs, v_refs, blocks, cols)
        for ref in before:
            part = part + ref[:, cols]
        out_ref[:, cols] = part


def forward_kernel(lanes, blocks, *refs):
    len_ref, q_ref = refs[:2]
    count = len(blocks)
    k_refs = dict(zip(blocks, refs[2 : 2 + count]))
    v_refs = dict(zip(blocks, refs[2 + count :]))
    near_ref, gate_ref, gain_ref = refs[2 + 2 * count : 5 + 2 * count]
    mixed_ref, mixed_t_ref, normed_ref, inv_ref, att = refs[5 + 2 * count :]
    length = len_ref[0]
    for cols in pair_slices(q_ref.shape[1]):
        att[:, cols] = near_ref[:, cols] + attend(
            lanes, length, q_ref, k_refs, v_refs, blocks, cols
        )
    attended = att[...]
    centre = attended - jnp.mean(attended, axis=1, keepdims=True)
    inv_std = lax.rsqrt(jnp.mean(centre * centre, axis=1, keepdims=True) + EPS)
    normed = centre * inv_std
    mixed = (normed * gain_ref[...] * gate_ref[...].astype(F32)).astype(BF16)
    mixed_t_ref[...] = mixed.T
    mixed_ref[...] = mixed
    normed_ref[...] = normed
    inv_ref[...] = jnp.broadcast_to(inv_std, inv_ref.shape)


def query_kernel(lanes, *refs):
    len_ref, q_ref = refs[:2]
    k_refs, v_refs = refs[2 : 2 + lanes], refs[2 + lanes : 2 + 2 * lanes]
    gate_ref, gain_ref, og_ref, normed_ref, inv_ref, mixed_ref, w_ref = refs[2 + 2 * lanes : 9 + 2 * lanes]
    lo_ref, dq_ref, gg_ref, gq_ref = refs[9 + 2 * lanes :]
    length = len_ref[0]
    rows, feats = q_ref.shape
    gain = gain_ref[...]
    normed = normed_ref[...]
    mixed_grad = dot(og_ref[...], w_ref[...], NT)
    gg_ref[...] = (mixed_grad * (normed * gain)).astype(BF16)
    normed_grad = mixed_grad * gate_ref[...].astype(F32) * gain
    grad = inv_ref[:, :1] * (
        normed_grad
        - jnp.mean(normed_grad, axis=1, keepdims=True)
        - normed * jnp.mean(normed_grad * normed, axis=1, keepdims=True)
    )
    gq_ref[:, :feats] = grad.astype(BF16)
    gq_ref[:, feats:] = q_ref[...]
    lo_ref[...] = dot(mixed_ref[...], w_ref[...]).astype(BF16)
    limit = limits(length, rows)
    for cols in pair_slices(feats):
        lhs = two_heads(q_ref[:, cols] * BF16(HALF_SCALE))
        grads = two_heads(gq_ref[:, cols])
        acc = None
        for blocks in tiles(range(lanes)):
            keys = stack(k_refs, blocks, cols)
            half = dot(lhs, keys, NT)
            prob_grad = dot(grads, stack(v_refs, blocks, cols), NT)
            live = places(blocks, lanes, rows) <= limit
            slope = weight_and_slope(half, live)[1]
            score_grad = (prob_grad * slope).astype(BF16)
            part = dot(score_grad, keys)
            acc = part if acc is None else acc + part
        dq_ref[:, cols] = (one_pair(acc) * HALF_SCALE).astype(BF16)


def key_kernel(lanes, *refs):
    len_ref, k_ref, v_ref = refs[:3]
    gq_refs = refs[3 : 3 + lanes]
    dk_ref, dv_ref = refs[3 + lanes :]
    length = len_ref[0]
    rows, feats = k_ref.shape
    pos = lax.axis_index("blk")
    mine = lax.rem(lax.broadcasted_iota(jnp.int32, (CORES * rows, 1), 0), rows) + pos * rows
    for p, cols in enumerate(pair_slices(feats)):
        lhs = two_heads(k_ref[:, cols] * BF16(HALF_SCALE))
        val = two_heads(v_ref[:, cols])
        q_cols = slice(feats + p * PAIR, feats + (p + 1) * PAIR)
        dk = dv = None
        for blocks in tiles(range(lanes)):
            queries = stack(gq_refs, blocks, q_cols)
            grads = stack(gq_refs, blocks, cols)
            half = dot(lhs, queries, NT)
            prob_grad = dot(val, grads, NT)
            where = places(blocks, lanes, rows)
            where = jnp.where(where < length, where, -1)
            live = mine <= where
            weight, slope = weight_and_slope(half, live)
            score_grad = (prob_grad * slope).astype(BF16)
            part_k, part_v = dot(score_grad, queries), dot(weight.astype(BF16), grads)
            dk = part_k if dk is None else dk + part_k
            dv = part_v if dv is None else dv + part_v
        dk_ref[:, cols] = (one_pair(dk) * HALF_SCALE).astype(BF16)
        dv_ref[:, cols] = one_pair(dv).astype(BF16)


def split(total_ref, digit, keep_ref, send_refs):
    size = 1 + len(send_refs)
    part = keep_ref.shape[0]
    mine = digit_of(digit)
    keep_ref[...] = total_ref[pl.ds(pl.multiple_of(mine * part, part), part), :]
    for k, ref in enumerate(send_refs, 1):
        at = target(mine, k, size)
        ref[...] = total_ref[pl.ds(pl.multiple_of(at * part, part), part), :].astype(BF16)


def product_kernel(lanes, digit, *refs):
    m_refs, o_refs = refs[:lanes], refs[lanes : 2 * lanes]
    outs, acc = refs[2 * lanes : -1], refs[-1]
    width = acc.shape[1]
    first = lax.rem(lax.axis_index("blk"), CORES) == 0
    total = None
    for n in range(0, lanes, CORES):
        lhs = jnp.concatenate([m[...] for m in m_refs[n : n + CORES]], axis=1)
        rhs = jnp.concatenate([o[...] for o in o_refs[n : n + CORES]], axis=0)
        rhs = jnp.where(first, rhs[:, :width], rhs[:, width:])
        part = dot(lhs, rhs)
        total = part if total is None else total + part
    acc[...] = total
    split(acc, digit, outs[0], outs[1:])


def sum_split_kernel(count, whole, digit, *refs):
    outs, acc = refs[1 + count : -1], refs[-1]
    if whole is None:
        total = refs[0][...]
        for ref in refs[1 : 1 + count]:
            total = total + ref[...].astype(F32)
    else:
        mine, size = digit_of(whole), whole[1]
        rows = refs[0].shape[0]
        for k, ref in enumerate(refs[: 1 + count]):
            at = source(mine, k, size) * rows
            acc[pl.ds(pl.multiple_of(at, rows), rows), :] = ref[...].astype(F32)
        total = acc[:rows, :]
        for k in range(1, size):
            total = total + acc[k * rows : (k + 1) * rows, :]
        acc = acc.at[:rows, :]
    acc[...] = total
    if digit is None:
        outs[0][...] = total.astype(outs[0].dtype)
    else:
        split(acc, digit, outs[0], outs[1:])


def join_kernel(digit, *refs):
    parts, out = refs[:-1], refs[-1]
    size, part = len(parts), parts[0].shape[0]
    mine = digit_of(digit)
    for k, ref in enumerate(parts):
        at = source(mine, k, size)
        out[pl.ds(pl.multiple_of(at * part, part), part), :] = ref[...].astype(out.dtype)


def layer(query, key, value, gate_u, out_grad, lengths, norm_gain, out_weight):
    rows, feats = query.shape
    model = out_grad.shape[1]
    lanes = lax.axis_size("blk")
    groups = lax.axis_size("grp")
    chips = lanes // CORES
    total = rows * lanes
    width = model // lanes
    steps = range(1, chips)

    def cross(x):
        return [over_blk(x, lanes, k, 0) for k in steps]

    def cores(pieces):
        out = []
        for x in pieces:
            out += [x, over_blk(x, lanes, 0, 1)]
        return out

    keys = cores([key] + cross(key))
    values = cores([value] + cross(value))
    query_here, key_here, value_here, gates, *columns = call(
        functools.partial(fetch_kernel, chips),
        [((rows, feats), BF16)] * 4 + [((rows, model // chips), BF16)] * chips,
        *(pltpu.with_memory_space_constraint(x, pltpu.HBM) for x in (out_grad, query, key, value, gate_u)),
        scratch=[pltpu.SemaphoreType.DMA((4 + chips,))],
        space=pltpu.HBM,
    )
    keys[0], values[0] = key_here, value_here
    moved = [over_blk(columns[k], lanes, k, 0) for k in steps]
    columns = cores([columns[0]] + moved)

    attention_flops = 4 * rows * total * feats
    gain = norm_gain.reshape(1, feats)

    def share(blocks, *before):
        return call(
            functools.partial(partial_kernel, lanes, blocks),
            [((rows, feats), F32)],
            lengths,
            query_here,
            *(keys[n] for n in blocks),
            *(values[n] for n in blocks),
            *before,
            scalars=1,
            flops=attention_flops * len(blocks) // lanes,
        )

    attended = share(list(range(CORES)))
    last = list(range(CORES + 1, lanes, CORES))
    if last:
        attended = share(list(range(CORES, lanes, CORES)), *attended)
    mixed, mixed_t, normed, inv_std = call(
        functools.partial(forward_kernel, lanes, last),
        [
            ((rows, feats), BF16),
            ((feats, rows), BF16),
            ((rows, feats), F32),
            ((rows, PAIR), F32),
        ],
        lengths,
        query_here,
        *(keys[n] for n in last),
        *(values[n] for n in last),
        *attended,
        gates,
        gain,
        scalars=1,
        scratch=[pltpu.VMEM((rows, feats), F32)],
        flops=attention_flops * len(last) // lanes,
    )
    mixes = cores([mixed_t] + cross(mixed_t))
    layer_out, grad_query, grad_gate, grads_queries = call(
        functools.partial(query_kernel, lanes),
        [
            ((rows, model), BF16),
            ((rows, feats), BF16),
            ((rows, feats), BF16),
            ((rows, 2 * feats), BF16),
        ],
        lengths,
        query_here,
        *keys,
        *values,
        gates,
        gain,
        out_grad,
        normed,
        inv_std,
        mixed,
        out_weight,
        scalars=1,
        flops=attention_flops + 4 * rows * feats * model,
    )
    grads = cores([grads_queries] + cross(grads_queries))
    grad_key, grad_value = call(
        functools.partial(key_kernel, lanes),
        [((rows, feats), BF16), ((rows, feats), BF16)],
        lengths,
        key_here,
        value_here,
        *grads,
        scalars=1,
        flops=2 * attention_flops,
    )

    stages = digits(groups)
    size = feats
    plan = []
    for n, digit in enumerate(stages):
        parts = digit[1] if n == 0 and size % (16 * digit[1]) == 0 else 1
        size //= parts
        plan.append((digit, parts, size))

    def pieces_of(parts, part):
        return [((part, width), F32)] + [((part, width), BF16)] * (parts - 1)

    held = call(
        functools.partial(product_kernel, lanes, plan[0][0]),
        pieces_of(plan[0][1], plan[0][2]),
        *mixes,
        *columns,
        scratch=[pltpu.VMEM((feats, width), F32)],
        flops=2 * total * feats * width,
    )
    for n, (digit, parts, part) in enumerate(plan):
        if parts > 1:
            received = [over_digit(held[k], groups, digit, k) for k in range(1, parts)]
        else:
            held = [held[0].astype(BF16)]
            received = [over_digit(held[0], groups, digit, k) for k in range(1, digit[1])]
        last = n + 1 == len(plan)
        nxt = None if last else plan[n + 1]
        split_next = not last and nxt[1] > 1
        held = call(
            functools.partial(
                sum_split_kernel,
                len(received),
                None if parts > 1 else digit,
                nxt[0] if split_next else None,
            ),
            [((part, width), BF16)] if not split_next else pieces_of(nxt[1], nxt[2]),
            held[0],
            *received,
            scratch=[pltpu.VMEM((part if parts > 1 else part * digit[1], width), F32)],
        )
    piece = held[0]
    gathers = [entry for entry in plan[::-1] if entry[1] > 1]
    for n, (digit, parts, part) in enumerate(gathers):
        received = [over_digit(piece, groups, digit, k) for k in range(1, parts)]
        (piece,) = call(
            functools.partial(join_kernel, digit),
            [((part * parts, width), F32 if n + 1 == len(gathers) else BF16)],
            piece,
            *received,
        )
    return (layer_out, grad_query, grad_key, grad_value, grad_gate, piece.astype(F32))


def solution(mesh):
    rows = P(("grp", "blk"), None)
    return jax.shard_map(
        layer,
        mesh=mesh,
        in_specs=(rows, rows, rows, rows, rows, P("grp"), P(), P()),
        out_specs=(rows, rows, rows, rows, rows, P(None, "blk")),
        check_vma=False,
    )
```

```python
import functools
import math

import jax
import jax.numpy as jnp
from jax import lax
from jax.experimental import pallas as pl
from jax.experimental.pallas import tpu as pltpu
from jax.sharding import PartitionSpec as P


HEAD = 64
PAIR = 2 * HEAD
EPS = 1e-05
F32 = jnp.float32
BF16 = jnp.bfloat16
CORES = 2
WORK_BYTES = 8 << 20

NT = (((1,), (1,)), ((), ()))
NN = (((1,), (0,)), ((), ()))


def dot(a, b, dims=NN):
    return lax.dot_general(a, b, dims, preferred_element_type=F32)


def nbytes(shape, dtype):
    return math.prod(shape) * jnp.dtype(dtype).itemsize


def call(kernel, outs, *args, scalars=0, scratch=(), flops=0, space=pltpu.VMEM):
    smem = pl.BlockSpec(memory_space=pltpu.SMEM)
    vmem = pl.BlockSpec(memory_space=pltpu.VMEM)
    inputs = pl.BlockSpec(memory_space=space)
    held = sum(nbytes(x.shape, x.dtype) for x in args) + sum(nbytes(*o) for o in outs)
    held += sum(nbytes(x.shape, x.dtype) for x in scratch if x.memory_space == pltpu.VMEM)
    return pl.pallas_call(
        kernel,
        out_shape=[jax.ShapeDtypeStruct(s, d) for s, d in outs],
        in_specs=[smem] * scalars + [inputs] * (len(args) - scalars),
        out_specs=[vmem] * len(outs),
        scratch_shapes=list(scratch),
        cost_estimate=pl.CostEstimate(flops=flops, transcendentals=0, bytes_accessed=0),
        compiler_params=pltpu.CompilerParams(vmem_limit_bytes=held + WORK_BYTES),
    )(*args)


def is_pow2(size):
    return size & (size - 1) == 0


def target(index, k, size):
    if is_pow2(size):
        return index ^ k
    return (index + k) % size if isinstance(index, int) else lax.rem(index + k, size)


def source(index, k, size):
    if is_pow2(size):
        return index ^ k
    return (index - k) % size if isinstance(index, int) else lax.rem(index + size - k, size)


def over_blk(x, lanes, step, other):
    chips = lanes // CORES
    pairs = []
    for i in range(lanes):
        chip, core = divmod(i, CORES)
        pairs.append((i, target(chip, step, chips) * CORES + (core + other) % CORES))
    return lax.ppermute(x, "blk", pairs)


def digits(groups):
    out, stride = [], 1
    for size in [4] + [2] * groups:
        if groups // stride % size == 0:
            out.append((stride, size))
            stride *= size
    if groups // stride > 1:
        out.append((stride, groups // stride))
    return out


def over_digit(x, groups, digit, k):
    stride, size = digit
    pairs = []
    for i in range(groups):
        d = (i // stride) % size
        pairs.append((i, i + (target(d, k, size) - d) * stride))
    return lax.ppermute(x, "grp", pairs)


def digit_of(digit):
    stride, size = digit
    return lax.rem(lax.div(lax.axis_index("grp"), jnp.int32(stride)), jnp.int32(size))


def low_lanes(shape):
    return lax.broadcasted_iota(jnp.int32, shape, 1) < HEAD


def two_heads(x):
    low = low_lanes(x.shape)
    zero = jnp.zeros_like(x)
    return jnp.concatenate([jnp.where(low, x, zero), jnp.where(low, zero, x)], axis=0)


def one_pair(x):
    rows = x.shape[0] // 2
    top, bottom = x[:rows], x[rows:]
    return jnp.where(low_lanes(top.shape), top, bottom)


def block_at(n, lanes):
    chips = lanes // CORES
    pos = lax.axis_index("blk")
    chip, core = lax.div(pos, CORES), lax.rem(pos, CORES)
    return source(chip, n // CORES, chips) * CORES + lax.rem(core + n % CORES, CORES)


def tiles(blocks, size=4):
    return [blocks[n : n + size] for n in range(0, len(blocks), size)]


def places(blocks, lanes, rows):
    lane = lax.broadcasted_iota(jnp.int32, (1, rows), 1)
    return jnp.concatenate([block_at(n, lanes) * rows + lane for n in blocks], axis=1)


def limits(length, rows):
    pos = lax.axis_index("blk")
    local = lax.rem(lax.broadcasted_iota(jnp.int32, (CORES * rows, 1), 0), rows)
    row = local + pos * rows
    return jnp.where(row < length, row, -1)


def stack(refs, blocks, cols):
    return jnp.concatenate([refs[n][:, cols] for n in blocks], axis=0)


def pair_slices(feats):
    return [slice(p * PAIR, (p + 1) * PAIR) for p in range(feats // PAIR)]


HALF_SCALE = HEAD ** -0.5 / 2


def fetch_kernel(chips, og_ref, *refs):
    count = (len(refs) - chips - 1) // 2
    sources, outs, sem = list(refs[:count]), refs[count:-1], refs[-1]
    chip = lax.div(lax.axis_index("blk"), CORES)
    width = outs[-1].shape[1]
    for k in range(chips):
        at = pl.multiple_of(target(chip, k, chips) * width, width)
        sources.append(og_ref.at[:, pl.ds(at, width)])
    copies = [
        pltpu.make_async_copy(src, dst, sem.at[n]) for n, (src, dst) in enumerate(zip(sources, outs))
    ]
    for copy in copies:
        copy.start()
    for copy in copies:
        copy.wait()


def weight_and_slope(half, live):
    u = jnp.where(live, 1.0 + jnp.tanh(half), 0.0)
    weight = half * u
    return weight, u + weight * (2.0 - u)


def attend(lanes, length, q_ref, k_refs, v_refs, blocks, cols):
    rows = q_ref.shape[0]
    lhs = two_heads(q_ref[:, cols] * BF16(HALF_SCALE))
    limit = limits(length, rows)
    acc = None
    for some in tiles(blocks):
        half = dot(lhs, stack(k_refs, some, cols), NT)
        live = places(some, lanes, rows) <= limit
        weight = jnp.where(live, half + half * jnp.tanh(half), 0.0).astype(BF16)
        part = dot(weight, stack(v_refs, some, cols))
        acc = part if acc is None else acc + part
    return one_pair(acc)


def partial_kernel(lanes, blocks, *refs):
    len_ref, q_ref = refs[:2]
    k_refs = dict(zip(blocks, refs[2 : 2 + len(blocks)]))
    v_refs = dict(zip(blocks, refs[2 + len(blocks) :]))
    before, out_ref = refs[2 + 2 * len(blocks) : -1], refs[-1]
    length = len_ref[0]
    for cols in pair_slices(q_ref.shape[1]):
        part = attend(lanes, length, q_ref, k_refs, v_refs, blocks, cols)
        for ref in before:
            part = part + ref[:, cols]
        out_ref[:, cols] = part


def forward_kernel(lanes, blocks, *refs):
    len_ref, q_ref = refs[:2]
    count = len(blocks)
    k_refs = dict(zip(blocks, refs[2 : 2 + count]))
    v_refs = dict(zip(blocks, refs[2 + count :]))
    near_ref, gate_ref, gain_ref = refs[2 + 2 * count : 5 + 2 * count]
    mixed_ref, mixed_t_ref, normed_ref, inv_ref, att = refs[5 + 2 * count :]
    length = len_ref[0]
    for cols in pair_slices(q_ref.shape[1]):
        att[:, cols] = near_ref[:, cols] + attend(
            lanes, length, q_ref, k_refs, v_refs, blocks, cols
        )
    attended = att[...]
    centre = attended - jnp.mean(attended, axis=1, keepdims=True)
    inv_std = lax.rsqrt(jnp.mean(centre * centre, axis=1, keepdims=True) + EPS)
    normed = centre * inv_std
    mixed = (normed * gain_ref[...] * gate_ref[...].astype(F32)).astype(BF16)
    mixed_t_ref[...] = mixed.T
    mixed_ref[...] = mixed
    normed_ref[...] = normed
    inv_ref[...] = jnp.broadcast_to(inv_std, inv_ref.shape)


def query_kernel(lanes, *refs):
    len_ref, q_ref = refs[:2]
    k_refs, v_refs = refs[2 : 2 + lanes], refs[2 + lanes : 2 + 2 * lanes]
    gate_ref, gain_ref, og_ref, normed_ref, inv_ref, mixed_ref, w_ref = refs[2 + 2 * lanes : 9 + 2 * lanes]
    lo_ref, dq_ref, gg_ref, gq_ref = refs[9 + 2 * lanes :]
    length = len_ref[0]
    rows, feats = q_ref.shape
    gain = gain_ref[...]
    normed = normed_ref[...]
    mixed_grad = dot(og_ref[...], w_ref[...], NT)
    gg_ref[...] = (mixed_grad * (normed * gain)).astype(BF16)
    normed_grad = mixed_grad * gate_ref[...].astype(F32) * gain
    grad = inv_ref[:, :1] * (
        normed_grad
        - jnp.mean(normed_grad, axis=1, keepdims=True)
        - normed * jnp.mean(normed_grad * normed, axis=1, keepdims=True)
    )
    gq_ref[:, :feats] = grad.astype(BF16)
    gq_ref[:, feats:] = q_ref[...]
    lo_ref[...] = dot(mixed_ref[...], w_ref[...]).astype(BF16)
    limit = limits(length, rows)
    for cols in pair_slices(feats):
        lhs = two_heads(q_ref[:, cols] * BF16(HALF_SCALE))
        grads = two_heads(gq_ref[:, cols])
        acc = None
        for blocks in tiles(range(lanes)):
            keys = stack(k_refs, blocks, cols)
            half = dot(lhs, keys, NT)
            prob_grad = dot(grads, stack(v_refs, blocks, cols), NT)
            live = places(blocks, lanes, rows) <= limit
            slope = weight_and_slope(half, live)[1]
            score_grad = (prob_grad * slope).astype(BF16)
            part = dot(score_grad, keys)
            acc = part if acc is None else acc + part
        dq_ref[:, cols] = (one_pair(acc) * HALF_SCALE).astype(BF16)


def key_kernel(lanes, blocks, *refs):
    len_ref, k_ref, v_ref = refs[:3]
    count = len(blocks)
    gq_refs = dict(zip(blocks, refs[3 : 3 + count]))
    before, outs = refs[3 + count : -2], refs[-2:]
    length = len_ref[0]
    rows, feats = k_ref.shape
    pos = lax.axis_index("blk")
    mine = lax.rem(lax.broadcasted_iota(jnp.int32, (CORES * rows, 1), 0), rows) + pos * rows
    for p, cols in enumerate(pair_slices(feats)):
        lhs = two_heads(k_ref[:, cols] * BF16(HALF_SCALE))
        val = two_heads(v_ref[:, cols])
        q_cols = slice(feats + p * PAIR, feats + (p + 1) * PAIR)
        dk = dv = None
        for some in tiles(blocks):
            queries = stack(gq_refs, some, q_cols)
            grads = stack(gq_refs, some, cols)
            half = dot(lhs, queries, NT)
            prob_grad = dot(val, grads, NT)
            where = places(some, lanes, rows)
            live = mine <= jnp.where(where < length, where, -1)
            weight, slope = weight_and_slope(half, live)
            score_grad = (prob_grad * slope).astype(BF16)
            part_k, part_v = dot(score_grad, queries), dot(weight.astype(BF16), grads)
            dk = part_k if dk is None else dk + part_k
            dv = part_v if dv is None else dv + part_v
        for out, grad, ref, scale in zip(outs, (dk, dv), before or (None, None), (HALF_SCALE, 1.0)):
            grad = one_pair(grad)
            if ref is not None:
                grad = grad + ref[:, cols]
            out[:, cols] = grad if out.dtype == F32 else (grad * scale).astype(out.dtype)


def split(total_ref, digit, keep_ref, send_refs):
    size = 1 + len(send_refs)
    part = keep_ref.shape[0]
    mine = digit_of(digit)
    keep_ref[...] = total_ref[pl.ds(pl.multiple_of(mine * part, part), part), :]
    for k, ref in enumerate(send_refs, 1):
        at = target(mine, k, size)
        ref[...] = total_ref[pl.ds(pl.multiple_of(at * part, part), part), :].astype(BF16)


def product_kernel(lanes, digit, *refs):
    m_refs, o_refs = refs[:lanes], refs[lanes : 2 * lanes]
    outs, acc = refs[2 * lanes : -1], refs[-1]
    width = acc.shape[1]
    first = lax.rem(lax.axis_index("blk"), CORES) == 0
    total = None
    for n in range(0, lanes, CORES):
        lhs = jnp.concatenate([m[...] for m in m_refs[n : n + CORES]], axis=1)
        rhs = jnp.concatenate([o[...] for o in o_refs[n : n + CORES]], axis=0)
        rhs = jnp.where(first, rhs[:, :width], rhs[:, width:])
        part = dot(lhs, rhs)
        total = part if total is None else total + part
    acc[...] = total
    split(acc, digit, outs[0], outs[1:])


def sum_split_kernel(count, whole, digit, *refs):
    outs, acc = refs[1 + count : -1], refs[-1]
    if whole is None:
        total = refs[0][...]
        for ref in refs[1 : 1 + count]:
            total = total + ref[...].astype(F32)
    else:
        mine, size = digit_of(whole), whole[1]
        rows = refs[0].shape[0]
        for k, ref in enumerate(refs[: 1 + count]):
            at = source(mine, k, size) * rows
            acc[pl.ds(pl.multiple_of(at, rows), rows), :] = ref[...].astype(F32)
        total = acc[:rows, :]
        for k in range(1, size):
            total = total + acc[k * rows : (k + 1) * rows, :]
        acc = acc.at[:rows, :]
    acc[...] = total
    if digit is None:
        outs[0][...] = total.astype(outs[0].dtype)
    else:
        split(acc, digit, outs[0], outs[1:])


def join_kernel(digit, *refs):
    parts, out = refs[:-1], refs[-1]
    size, part = len(parts), parts[0].shape[0]
    mine = digit_of(digit)
    for k, ref in enumerate(parts):
        at = source(mine, k, size)
        out[pl.ds(pl.multiple_of(at * part, part), part), :] = ref[...].astype(out.dtype)


def layer(query, key, value, gate_u, out_grad, lengths, norm_gain, out_weight):
    rows, feats = query.shape
    model = out_grad.shape[1]
    lanes = lax.axis_size("blk")
    groups = lax.axis_size("grp")
    chips = lanes // CORES
    total = rows * lanes
    width = model // lanes
    steps = range(1, chips)

    def cross(x):
        return [over_blk(x, lanes, k, 0) for k in steps]

    def cores(pieces):
        out = []
        for x in pieces:
            out += [x, over_blk(x, lanes, 0, 1)]
        return out

    keys = cores([key] + cross(key))
    values = cores([value] + cross(value))
    query_here, key_here, value_here, gates, *columns = call(
        functools.partial(fetch_kernel, chips),
        [((rows, feats), BF16)] * 4 + [((rows, model // chips), BF16)] * chips,
        *(pltpu.with_memory_space_constraint(x, pltpu.HBM) for x in (out_grad, query, key, value, gate_u)),
        scratch=[pltpu.SemaphoreType.DMA((4 + chips,))],
        space=pltpu.HBM,
    )
    keys[0], values[0] = key_here, value_here
    moved = [over_blk(columns[k], lanes, k, 0) for k in steps]
    columns = cores([columns[0]] + moved)

    attention_flops = 4 * rows * total * feats
    gain = norm_gain.reshape(1, feats)

    def share(blocks, *before):
        return call(
            functools.partial(partial_kernel, lanes, blocks),
            [((rows, feats), F32)],
            lengths,
            query_here,
            *(keys[n] for n in blocks),
            *(values[n] for n in blocks),
            *before,
            scalars=1,
            flops=attention_flops * len(blocks) // lanes,
        )

    attended = share(list(range(CORES)))
    last = list(range(CORES + 1, lanes, CORES))
    if last:
        attended = share(list(range(CORES, lanes, CORES)), *attended)
    mixed, mixed_t, normed, inv_std = call(
        functools.partial(forward_kernel, lanes, last),
        [
            ((rows, feats), BF16),
            ((feats, rows), BF16),
            ((rows, feats), F32),
            ((rows, PAIR), F32),
        ],
        lengths,
        query_here,
        *(keys[n] for n in last),
        *(values[n] for n in last),
        *attended,
        gates,
        gain,
        scalars=1,
        scratch=[pltpu.VMEM((rows, feats), F32)],
        flops=attention_flops * len(last) // lanes,
    )
    mixes = cores([mixed_t] + cross(mixed_t))
    layer_out, grad_query, grad_gate, grads_queries = call(
        functools.partial(query_kernel, lanes),
        [
            ((rows, model), BF16),
            ((rows, feats), BF16),
            ((rows, feats), BF16),
            ((rows, 2 * feats), BF16),
        ],
        lengths,
        query_here,
        *keys,
        *values,
        gates,
        gain,
        out_grad,
        normed,
        inv_std,
        mixed,
        out_weight,
        scalars=1,
        flops=attention_flops + 4 * rows * feats * model,
    )
    grads = cores([grads_queries] + cross(grads_queries))

    def key_share(blocks, kind, *before):
        return call(
            functools.partial(key_kernel, lanes, blocks),
            [((rows, feats), kind)] * 2,
            lengths,
            key_here,
            value_here,
            *(grads[n] for n in blocks),
            *before,
            scalars=1,
            flops=2 * attention_flops * len(blocks) // lanes,
        )

    here, away = list(range(CORES)), list(range(CORES, lanes))
    shares = key_share(here, F32) if away else []
    grad_key, grad_value = key_share(away or here, BF16, *shares)

    stages = digits(groups)
    size = feats
    plan = []
    for n, digit in enumerate(stages):
        parts = digit[1] if n == 0 and size % (16 * digit[1]) == 0 else 1
        size //= parts
        plan.append((digit, parts, size))

    def pieces_of(parts, part):
        return [((part, width), F32)] + [((part, width), BF16)] * (parts - 1)

    held = call(
        functools.partial(product_kernel, lanes, plan[0][0]),
        pieces_of(plan[0][1], plan[0][2]),
        *mixes,
        *columns,
        scratch=[pltpu.VMEM((feats, width), F32)],
        flops=2 * total * feats * width,
    )
    for n, (digit, parts, part) in enumerate(plan):
        if parts > 1:
            received = [over_digit(held[k], groups, digit, k) for k in range(1, parts)]
        else:
            held = [held[0].astype(BF16)]
            received = [over_digit(held[0], groups, digit, k) for k in range(1, digit[1])]
        last = n + 1 == len(plan)
        nxt = None if last else plan[n + 1]
        split_next = not last and nxt[1] > 1
        held = call(
            functools.partial(
                sum_split_kernel,
                len(received),
                None if parts > 1 else digit,
                nxt[0] if split_next else None,
            ),
            [((part, width), BF16)] if not split_next else pieces_of(nxt[1], nxt[2]),
            held[0],
            *received,
            scratch=[pltpu.VMEM((part if parts > 1 else part * digit[1], width), F32)],
        )
    piece = held[0]
    gathers = [entry for entry in plan[::-1] if entry[1] > 1]
    for n, (digit, parts, part) in enumerate(gathers):
        received = [over_digit(piece, groups, digit, k) for k in range(1, parts)]
        (piece,) = call(
            functools.partial(join_kernel, digit),
            [((part * parts, width), F32 if n + 1 == len(gathers) else BF16)],
            piece,
            *received,
        )
    return (layer_out, grad_query, grad_key, grad_value, grad_gate, piece.astype(F32))


def solution(mesh):
    rows = P(("grp", "blk"), None)
    return jax.shard_map(
        layer,
        mesh=mesh,
        in_specs=(rows, rows, rows, rows, rows, P("grp"), P(), P()),
        out_specs=(rows, rows, rows, rows, rows, P(None, "blk")),
        check_vma=False,
    )
```
